32 devices in a mesh: tp: 4 (over z), dp: 8 (over y, x, core).
Axes of the slice: x: 2, y: 2, z: 4, core: 2. Of those that a mesh axis runs over, the one named last changes fastest.
Arguments:
- hidden: bfloat16 [8, 1024, 768], P('dp')
- ln_gamma: float32 [768], replicated
- ln_beta: float32 [768], replicated
- embed_table: bfloat16 [50272, 768], P('tp')
- labels: int32 [8, 1024], P('dp')
- loss_mask: int32 [8, 1024], P('dp')
Outputs:
- output 1: float32 [], replicated
- output 2: bfloat16 [8, 1024, 768], P('dp')
- output 3: float32 [50272, 768], P('tp')
- output 4: float32 [768], replicated
- output 5: float32 [768], replicated
All inputs are finite; a program needn't handle non-finite values.
Results may differ from the reference program's by a relative error of at most 0.001.
Values sent between devices are 32-bit elements.
A program may use at most 1 GiB of HBM per device.

```python
import jax
import jax.numpy as jnp
from jax import lax

HIDDEN = 768
VOCAB_SIZE = 50272
NUM_SEQS = 8
SEQ_LEN = 1024
TOKEN_BLOCK = min(SEQ_LEN, 128)
LAYER_EPS = 1e-5
SCORE_SCALE = 3.5


def setup_inputs(seed: int = 0) -> dict:
    rand_keys = jax.random.split(jax.random.key(seed), 6)
    hidden = (1.5 * jax.random.normal(rand_keys[0], (NUM_SEQS, SEQ_LEN, HIDDEN), jnp.float32)).astype(jnp.bfloat16)
    ln_gamma = 1.0 + 0.3 * jax.random.normal(rand_keys[1], (HIDDEN,), jnp.float32)
    ln_beta = 0.3 * jax.random.normal(rand_keys[2], (HIDDEN,), jnp.float32)
    embed_table = (SCORE_SCALE * HIDDEN ** -0.5 * jax.random.normal(rand_keys[3], (VOCAB_SIZE, HIDDEN), jnp.float32)).astype(jnp.bfloat16)
    labels = jax.random.randint(rand_keys[4], (NUM_SEQS, SEQ_LEN), 0, VOCAB_SIZE, jnp.int32)
    lengths = jax.random.randint(rand_keys[5], (NUM_SEQS, 1), 1, SEQ_LEN + 1, jnp.int32)
    positions = jnp.arange(SEQ_LEN, dtype=jnp.int32)[None, :]
    loss_mask = (positions < lengths).astype(jnp.int32)
    return {'hidden': hidden, 'ln_gamma': ln_gamma, 'ln_beta': ln_beta, 'embed_table': embed_table, 'labels': labels, 'loss_mask': loss_mask}


def reference(hidden, ln_gamma, ln_beta, embed_table, labels, loss_mask):
    mask_float = loss_mask.astype(jnp.float32)
    token_count = jnp.sum(mask_float)
    vocab_ids = jnp.arange(VOCAB_SIZE, dtype=jnp.int32)[None, :]
    block_hidden = hidden.reshape(-1, TOKEN_BLOCK, HIDDEN)
    block_labels = labels.reshape(-1, TOKEN_BLOCK)
    block_mask = mask_float.reshape(-1, TOKEN_BLOCK, 1)

    def block_step(scan_carry, block_data):
        d_embed, d_gamma, d_beta, loss_sum = scan_carry
        block_rows, row_labels, row_mask = block_data
        x_float = block_rows.astype(jnp.float32)
        row_mean = jnp.mean(x_float, axis=-1, keepdims=True)
        centered = x_float - row_mean
        inv_std = lax.rsqrt(jnp.mean(centered * centered, axis=-1, keepdims=True) + LAYER_EPS)
        x_hat = centered * inv_std
        normed = (x_hat * ln_gamma + ln_beta).astype(jnp.bfloat16)
        logits = jnp.dot(normed, embed_table.T, preferred_element_type=jnp.float32)
        row_max = jnp.max(logits, axis=-1, keepdims=True)
        log_norm = row_max + jnp.log(jnp.sum(jnp.exp(logits - row_max), axis=-1, keepdims=True))
        is_target = vocab_ids == row_labels[:, None]
        target_logit = jnp.sum(jnp.where(is_target, logits, 0.0), axis=-1, keepdims=True)
        loss_sum = loss_sum + jnp.sum(row_mask * (log_norm - target_logit))
        soft_probs = jnp.exp(logits - log_norm)
        grad_logits = (jnp.where(is_target, soft_probs - 1.0, soft_probs) * (row_mask / token_count)).astype(jnp.bfloat16)
        grad_normed = jnp.dot(grad_logits, embed_table, preferred_element_type=jnp.float32)
        d_embed = d_embed + jnp.dot(grad_logits.T, normed, preferred_element_type=jnp.float32)
        d_gamma = d_gamma + jnp.sum(grad_normed * x_hat, axis=0)
        d_beta = d_beta + jnp.sum(grad_normed, axis=0)
        grad_scaled = grad_normed * ln_gamma
        grad_x = (grad_scaled - jnp.mean(grad_scaled, axis=-1, keepdims=True) - x_hat * jnp.mean(grad_scaled * x_hat, axis=-1, keepdims=True)) * inv_std
        return (d_embed, d_gamma, d_beta, loss_sum), grad_x.astype(jnp.bfloat16)

    zero_carry = (jnp.zeros((VOCAB_SIZE, HIDDEN), jnp.float32), jnp.zeros((HIDDEN,), jnp.float32), jnp.zeros((HIDDEN,), jnp.float32), jnp.zeros((), jnp.float32))
    final_carry, grad_blocks = lax.scan(block_step, zero_carry, (block_hidden, block_labels, block_mask))
    d_embed, d_gamma, d_beta, loss_sum = final_carry
    d_hidden = grad_blocks.reshape(NUM_SEQS, SEQ_LEN, HIDDEN)
    return loss_sum / token_count, d_hidden, d_embed, d_gamma, d_beta
```

```python
import jax
import jax.numpy as jnp
from jax import lax
from jax.experimental import pallas as pl
from jax.experimental.pallas import tpu as pltpu
from jax.sharding import PartitionSpec as P

LAYER_EPS = 1e-5
MESH = pl.DeviceIdType.MESH
F32, BF16 = jnp.float32, jnp.bfloat16
SEQ, WIDTH = 1024, 768
ROWS = 12568
BLOCK = 512
FULL = ROWS // BLOCK
REST = ROWS - FULL * BLOCK
RESTPAD = 384
CHUNK = 256
HALF = 512
A_ROWS, A_STEPS = 256, 4
B_ROWS, B_STEPS = 272, 8
A_TOTAL = 8 * A_ROWS * A_STEPS
TAIL = ROWS - A_TOTAL - 2 * B_ROWS * B_STEPS
TAIL_AT = ROWS - TAIL
R_MAX = B_ROWS + TAIL
VMEM_LIMIT = 67_043_328


def layer_norm_fwd(hidden, ln_gamma, ln_beta):
    x_float = hidden.astype(F32)
    row_mean = jnp.mean(x_float, axis=-1, keepdims=True)
    centered = x_float - row_mean
    inv_std = lax.rsqrt(jnp.mean(centered * centered, axis=-1, keepdims=True) + LAYER_EPS)
    x_hat = centered * inv_std
    return x_hat, inv_std, x_hat * ln_gamma + ln_beta


class Plane:
    def __init__(self):
        self.me = me = lax.axis_index('dp')
        self.core = lax.rem(me, 2)
        dx = 2 - 4 * lax.rem(lax.div(me, 2), 2)
        dy = 4 - 8 * lax.div(me, 4)
        self.x, self.y, self.diag = me + dx, me + dy, me + dx + dy
        self.pair = p = me + 1 - 2 * self.core
        self.pair_x, self.pair_y, self.pair_diag = p + dx, p + dy, p + dx + dy


class Gather:
    def __init__(self, plane, region, send_sems, recv_sems):
        self.p, self.region, self.s, self.r = plane, region, send_sems, recv_sems

    def copy(self, lane, q, src, dst, device):
        return pltpu.make_async_remote_copy(
            src_ref=src, dst_ref=dst, send_sem=self.s.at[lane, q], recv_sem=self.r.at[lane, q],
            device_id={'dp': device}, device_id_type=MESH)

    def pass_on(self, lane, q, owner, device):
        part = self.region(owner, q)
        self.copy(lane, q, part, part, device).start()

    def arrived(self, lane, q, owner):
        part = self.region(owner, q)
        self.copy(lane, q, part, part, self.p.pair).wait_recv()

    def sent(self, lane, q, owner):
        part = self.region(owner, q)
        self.copy(lane, q, part, part, self.p.pair).wait_send()

    def send_own(self, q, src):
        p = self.p
        for lane, device in ((1, p.x), (2, p.y), (0, p.pair)):
            self.copy(lane, q, src, self.region(p.me, q), device).start()

    def own_sent(self, q):
        for lane in (0, 1, 2):
            self.sent(lane, q, self.p.me)

    def forward(self, q):
        p = self.p
        self.arrived(1, q, p.x)
        self.pass_on(3, q, p.x, p.pair)

        @pl.when(lax.rem(q, 2) == 0)
        def _():
            self.pass_on(6, q, p.x, p.y)

        self.arrived(2, q, p.y)
        self.pass_on(4, q, p.y, p.pair)

        @pl.when(lax.rem(q, 2) == 1)
        def _():
            self.pass_on(6, q, p.y, p.x)

    def forward_diag(self, q):
        self.arrived(6, q, self.p.diag)
        self.pass_on(5, q, self.p.diag, self.p.pair)

    def finish(self, q):
        p = self.p
        for lane, owner in ((0, p.pair), (3, p.pair_x), (4, p.pair_y), (5, p.pair_diag)):
            self.arrived(lane, q, owner)
        for lane, owner in ((3, p.x), (4, p.y), (5, p.diag), (6, p.x)):
            self.sent(lane, q, owner)


def enter(me, tp):
    barrier = pltpu.get_barrier_semaphore()
    for o in range(1, 8):
        pl.semaphore_signal(barrier, inc=1, device_id={'dp': lax.rem(me + o, 8)}, device_id_type=MESH)
    for o in range(1, 4):
        pl.semaphore_signal(barrier, inc=1, device_id={'tp': lax.rem(tp + o, 4)}, device_id_type=MESH)
    pl.semaphore_wait(barrier, 10)


class Exchange:
    def __init__(self, axis, size, buf, send_sems, recv_sems):
        self.axis, self.size, self.buf, self.s, self.r = axis, size, buf, send_sems, recv_sems
        self.me = lax.axis_index(axis)

    def copy(self, o, src, slot):
        return pltpu.make_async_remote_copy(
            src_ref=src, dst_ref=self.buf.at[slot], send_sem=self.s.at[o], recv_sem=self.r.at[o],
            device_id={self.axis: lax.rem(self.me + o, self.size)}, device_id_type=MESH)

    def start(self, src):
        for o in range(1, self.size):
            self.copy(o, src, self.me).start()

    def wait(self, src):
        for o in range(1, self.size):
            self.copy(o, src, lax.rem(self.me + self.size - o, self.size)).wait_recv()
        for o in range(1, self.size):
            self.copy(o, src, self.me).wait_send()


def offsets(groups, lanes):
    return 8 * lax.broadcasted_iota(jnp.int32, (groups, 8, lanes), 0)


def own_tokens_kernel(z_ref, zf_ref, e_ref, info_ref, zall_ref, dzh_ref, info_out, lse_out, dz_ref, half_in,
                      logits, eslot, top, total, target, rows8, infobuf, stat, statbuf, lsend, lsebuf,
                      e_sem, half_s, half_r, zs, zr, info_s, info_r, stat_s, stat_r, lse_s, lse_r):
    plane = Plane()
    me, tp = plane.me, lax.axis_index('tp')
    enter(me, tp)

    def zregion(owner, q):
        return zall_ref.at[owner, pl.ds(pl.multiple_of(q * CHUNK, CHUNK), CHUNK), :]

    gather = Gather(plane, zregion, zs, zr)
    infos = Exchange('dp', 8, infobuf, info_s, info_r)
    infos.start(info_ref)
    for q in range(4):
        gather.send_own(q, zf_ref.at[pl.ds(q * CHUNK, CHUNK), :])
    infobuf[me] = info_ref[...]

    def fetch(j, slot):
        return pltpu.make_async_copy(
            e_ref.at[pl.ds(pl.multiple_of(j * BLOCK, BLOCK), BLOCK), :], eslot.at[slot], e_sem.at[slot])

    def fetch_rest(slot):
        return pltpu.make_async_copy(
            e_ref.at[pl.ds(FULL * BLOCK, REST), :], eslot.at[slot, pl.ds(0, REST), :], e_sem.at[slot])

    def blocks(body):
        fetch(0, 0).start()

        def step(j, _):
            slot = lax.rem(j, 2)
            fetch(j, slot).wait()

            @pl.when(j < FULL - 1)
            def _():
                fetch(j + 1, 1 - slot).start()

            @pl.when(j == FULL - 1)
            def _():
                eslot[1 - slot, pl.ds(272, RESTPAD - 272), :] = jnp.zeros((RESTPAD - 272, WIDTH), BF16)
                fetch_rest(1 - slot).start()

            body(pl.multiple_of(j * BLOCK, BLOCK), slot, BLOCK)
            return 0

        lax.fori_loop(0, FULL, step, 0)
        fetch_rest(FULL % 2).wait()
        body(FULL * BLOCK, FULL % 2, RESTPAD)

    sub = lax.broadcasted_iota(jnp.int32, (8, SEQ), 0)
    rows8[0] = jnp.broadcast_to(info_ref[2:3, :].astype(jnp.int32), (8, SEQ)) - sub
    top[...] = jnp.full((8, SEQ), -jnp.inf, F32)
    total[...] = jnp.zeros((8, SEQ), F32)
    target[...] = jnp.zeros((8, SEQ), F32)

    def forward_block(at, slot, n):
        e = eslot[slot, pl.ds(0, n), :]
        for t in range(4):
            cols = pl.ds(t * CHUNK, CHUNK)
            l = lax.dot_general(e, z_ref[cols, :], (((1,), (1,)), ((), ())), preferred_element_type=F32)
            if n != BLOCK:
                l = jnp.where(lax.broadcasted_iota(jnp.int32, (n, CHUNK), 0) < REST, l, -jnp.inf)
            logits[pl.ds(at, n), cols] = l
            l = l.reshape(n // 8, 8, CHUNK)
            old = top[:, cols]
            new = jnp.maximum(old, jnp.max(l, axis=0))
            top[:, cols] = new
            total[:, cols] = total[:, cols] * jnp.exp(old - new) + jnp.sum(jnp.exp(l - new[None]), axis=0)
            hit = offsets(n // 8, CHUNK) == (rows8[0, :, cols] - at)[None]
            target[:, cols] += jnp.sum(jnp.where(hit, l, 0.0), axis=0)

    blocks(forward_block)

    m1 = jnp.max(top[...], axis=0, keepdims=True)
    stat[0:1, :] = m1
    stat[1:2, :] = jnp.sum(total[...] * jnp.exp(top[...] - m1), axis=0, keepdims=True)
    stat[2:3, :] = jnp.sum(target[...], axis=0, keepdims=True)
    stats = Exchange('tp', 4, statbuf, stat_s, stat_r)
    stats.start(stat)
    statbuf[tp] = stat[...]
    infos.wait(info_ref)
    token_count = jnp.sum(infobuf[:, 1, :], keepdims=True)
    stats.wait(stat)
    m4 = jnp.max(statbuf[:, 0, :], axis=0, keepdims=True)
    s4 = jnp.sum(statbuf[:, 1, :] * jnp.exp(statbuf[:, 0, :] - m4), axis=0, keepdims=True)
    lse = m4 + jnp.log(s4)
    lsend[0:1, :] = lse
    lsend[1:2, :] = jnp.sum(statbuf[:, 2, :], axis=0, keepdims=True)
    lses = Exchange('dp', 8, lsebuf, lse_s, lse_r)
    lses.start(lsend)
    lsebuf[me] = lsend[...]
    top[...] = jnp.broadcast_to(lse, (8, SEQ))
    total[...] = jnp.broadcast_to(info_ref[1:2, :] / token_count, (8, SEQ))
    gather.forward(0)

    dz_ref[...] = jnp.zeros((SEQ, WIDTH), F32)

    def backward_block(at, slot, n):
        e = eslot[slot, pl.ds(0, n), :]
        for t in range(4):
            cols = pl.ds(t * CHUNK, CHUNK)
            l = logits[pl.ds(at, n), cols].reshape(n // 8, 8, CHUNK)
            p = jnp.exp(l - top[:, cols][None])
            hit = offsets(n // 8, CHUNK) == (rows8[0, :, cols] - at)[None]
            g = (jnp.where(hit, p - 1.0, p) * total[:, cols][None]).reshape(n, CHUNK).astype(BF16)
            dz_ref[cols, :] += lax.dot_general(g, e, (((0,), (0,)), ((), ())), preferred_element_type=F32)

    blocks(backward_block)

    mine = pl.multiple_of(lax.rem(tp, 2) * HALF, HALF)
    theirs = pl.multiple_of(HALF - lax.rem(tp, 2) * HALF, HALF)
    halves = pltpu.make_async_remote_copy(
        src_ref=dz_ref.at[pl.ds(theirs, HALF), :], dst_ref=half_in, send_sem=half_s, recv_sem=half_r,
        device_id={'tp': tp + 1 - 2 * lax.rem(tp, 2)}, device_id_type=MESH)
    halves.start()
    for q in range(1, 4):
        gather.forward(q)
    lses.wait(lsend)
    info_out[...] = infobuf[...]
    lse_out[...] = lsebuf[...]
    for q in range(4):
        gather.forward_diag(q)
    halves.wait()
    dzh_ref[...] = dz_ref[pl.ds(mine, HALF), :] + half_in[...]
    for q in range(4):
        gather.own_sent(q)
        gather.finish(q)


def own_tokens(z, zf, embed, info):
    return pl.pallas_call(
        own_tokens_kernel,
        name='own_tokens',
        out_shape=(
            jax.ShapeDtypeStruct((8, SEQ, WIDTH), F32),
            jax.ShapeDtypeStruct((HALF, WIDTH), F32),
            jax.ShapeDtypeStruct((8, 8, SEQ), F32),
            jax.ShapeDtypeStruct((8, 8, SEQ), F32),
        ),
        in_specs=[
            pl.BlockSpec(memory_space=pltpu.VMEM),
            pl.BlockSpec(memory_space=pl.ANY),
            pl.BlockSpec(memory_space=pl.ANY),
            pl.BlockSpec(memory_space=pltpu.VMEM),
        ],
        out_specs=(
            pl.BlockSpec(memory_space=pl.ANY),
            pl.BlockSpec(memory_space=pltpu.VMEM),
            pl.BlockSpec(memory_space=pltpu.VMEM),
            pl.BlockSpec(memory_space=pltpu.VMEM),
        ),
        scratch_shapes=[
            pltpu.VMEM((SEQ, WIDTH), F32),
            pltpu.VMEM((HALF, WIDTH), F32),
            pltpu.VMEM((FULL * BLOCK + RESTPAD, SEQ), F32),
            pltpu.VMEM((2, BLOCK, WIDTH), BF16),
            pltpu.VMEM((8, SEQ), F32),
            pltpu.VMEM((8, SEQ), F32),
            pltpu.VMEM((8, SEQ), F32),
            pltpu.VMEM((1, 8, SEQ), jnp.int32),
            pltpu.VMEM((8, 8, SEQ), F32),
            pltpu.VMEM((8, SEQ), F32),
            pltpu.VMEM((4, 8, SEQ), F32),
            pltpu.VMEM((8, SEQ), F32),
            pltpu.VMEM((8, 8, SEQ), F32),
            pltpu.SemaphoreType.DMA((2,)),
            pltpu.SemaphoreType.DMA,
            pltpu.SemaphoreType.DMA,
            pltpu.SemaphoreType.DMA((7, 4)),
            pltpu.SemaphoreType.DMA((7, 4)),
            pltpu.SemaphoreType.DMA((8,)),
            pltpu.SemaphoreType.DMA((8,)),
            pltpu.SemaphoreType.DMA((4,)),
            pltpu.SemaphoreType.DMA((4,)),
            pltpu.SemaphoreType.DMA((8,)),
            pltpu.SemaphoreType.DMA((8,)),
        ],
        compiler_params=pltpu.CompilerParams(collective_id=1, has_side_effects=True, vmem_limit_bytes=VMEM_LIMIT),
        cost_estimate=pl.CostEstimate(flops=4 * SEQ * ROWS * WIDTH, bytes_accessed=4 * ROWS * WIDTH, transcendentals=2 * SEQ * ROWS),
    )(z, zf, embed, info)


def all_tokens_kernel(z_ref, zall_ref, e_ref, info_ref, lse_ref, dz_ref, xhat_ref, inv_ref, gamma_ref, de_ref, dh_ref, sums_out,
                      far_in, dhh, zb, zslot, eslot, lbuf, stage, lse8, scale8, rows8, sums, sum4, sumbuf4, sumbuf8,
                      far_s, far_r, dh_sem, dh_s, dh_r, z_sem, e_sem, t_sem, l_sem, gs, gr, b_s, b_r, s4_s, s4_r, s8_s, s8_r):
    plane = Plane()
    me, tp = plane.me, lax.axis_index('tp')
    enter(me, tp)

    def fetch(at, n, slot):
        return pltpu.make_async_copy(e_ref.at[pl.ds(at, n), :], eslot.at[slot, pl.ds(0, n), :], e_sem.at[slot])

    def a_at(owner, q):
        return pl.multiple_of((owner * A_STEPS + q) * A_ROWS, A_ROWS)

    def b_at(core, b):
        return pl.multiple_of(A_TOTAL + (core * B_STEPS + b) * B_ROWS, 16)

    fetch(a_at(me, 0), A_ROWS, 0).start()
    tail = pltpu.make_async_copy(e_ref.at[pl.ds(TAIL_AT, TAIL), :], eslot.at[2, pl.ds(B_ROWS, TAIL), :], t_sem)
    tail.start()

    mine = pl.multiple_of(lax.rem(tp, 2) * HALF, HALF)
    far = pltpu.make_async_remote_copy(
        src_ref=dz_ref, dst_ref=far_in, send_sem=far_s, recv_sem=far_r,
        device_id={'tp': lax.rem(tp + 2, 4)}, device_id_type=MESH)
    far.start()

    def column_sums(i, carry):
        at = pl.multiple_of(i * 128, 128)
        dz = dz_ref[pl.ds(at, 128), :]
        dzx = dz * xhat_ref[pl.ds(mine + at, 128), :]
        return carry[0] + jnp.sum(dzx.reshape(16, 8, WIDTH), axis=0), carry[1] + jnp.sum(dz.reshape(16, 8, WIDTH), axis=0)

    zero = jnp.zeros((8, WIDTH), F32)
    dgamma, dbeta = lax.fori_loop(0, 4, column_sums, (zero, zero))
    sums[0:8, :] = dgamma
    sums[8:16, :] = dbeta
    over_tp = Exchange('tp', 4, sumbuf4, s4_s, s4_r)
    over_tp.start(sums)
    sumbuf4[tp] = sums[...]

    def fetch_z(n):
        owner = lax.rem(me + 1 + lax.div(n, 4), 8)
        q = pl.multiple_of(lax.rem(n, 4) * CHUNK, CHUNK)
        slot = lax.rem(n, 4)
        return owner, q, slot, pltpu.make_async_copy(zall_ref.at[owner, pl.ds(q, CHUNK), :], zslot.at[slot], z_sem.at[slot])

    for n in range(3):
        fetch_z(n)[3].start()
    zb[me] = z_ref[...]
    token_count = jnp.sum(info_ref[:, 1, :], keepdims=True)
    sub = lax.broadcasted_iota(jnp.int32, (8, SEQ), 0) + tp * ROWS
    for s in range(8):
        lse8[s] = jnp.broadcast_to(lse_ref[s, 0:1, :], (8, SEQ))
        scale8[s] = jnp.broadcast_to(info_ref[s, 1:2, :] / token_count, (8, SEQ))
        rows8[s] = jnp.broadcast_to(info_ref[s, 0:1, :].astype(jnp.int32), (8, SEQ)) - sub

    def convert(n, _):
        owner, q, slot, copy = fetch_z(n)
        copy.wait()

        @pl.when(n < 25)
        def _():
            fetch_z(n + 3)[3].start()

        zb[owner, pl.ds(q, CHUNK), :] = zslot[slot].astype(BF16)
        return 0

    lax.fori_loop(0, 28, convert, 0)

    def logits_of(slot, n, s):
        return lax.dot_general(eslot[slot, pl.ds(0, n), :], zb[s], (((1,), (1,)), ((), ())), preferred_element_type=F32)

    def grad_of(l, n, s, at, tail_at):
        l = l.reshape(n // 8, 8, SEQ)
        p = jnp.exp(l - lse8[s][None])
        row = offsets(n // 8, SEQ) + at
        if tail_at is not None:
            row = jnp.where(offsets(n // 8, SEQ) < B_ROWS, row, row + (tail_at - B_ROWS - at))
        g = jnp.where(row == rows8[s][None], p - 1.0, p) * scale8[s][None]
        return g.reshape(n, SEQ).astype(BF16)

    def compute(slot, out, n, at, tail_at=None):
        lbuf[0, pl.ds(0, n), :] = logits_of(slot, n, 0)
        stage[out, pl.ds(0, n), :] = jnp.zeros((n, WIDTH), F32)

        def one(s, k, last):
            if not last:
                lbuf[1 - k, pl.ds(0, n), :] = logits_of(slot, n, s + 1)
            g = grad_of(lbuf[k, pl.ds(0, n), :], n, s, at, tail_at)
            stage[out, pl.ds(0, n), :] += jnp.dot(g, zb[s], preferred_element_type=F32)

        def pairs(i, _):
            one(2 * i, 0, False)
            one(2 * i + 1, 1, False)
            return 0

        lax.fori_loop(0, 3, pairs, 0)
        one(6, 0, False)
        one(7, 1, True)

    def region(owner, q):
        return de_ref.at[pl.ds(a_at(owner, q), A_ROWS), :]

    gather = Gather(plane, region, gs, gr)

    def keep(out, n, at):
        return pltpu.make_async_copy(stage.at[out, pl.ds(0, n), :], de_ref.at[pl.ds(at, n), :], l_sem.at[out])

    def a_step(q, _):
        slot = lax.rem(q, 2)
        fetch(a_at(me, q), A_ROWS, slot).wait()

        @pl.when(q < A_STEPS - 1)
        def _():
            fetch(a_at(me, q + 1), A_ROWS, 1 - slot).start()

        @pl.when(q == A_STEPS - 1)
        def _():
            fetch(b_at(plane.core, 0), B_ROWS, 1 - slot).start()

        compute(slot, 2 + q, A_ROWS, a_at(me, q))
        keep(2 + q, A_ROWS, a_at(me, q)).start()
        gather.send_own(q, stage.at[2 + q, pl.ds(0, A_ROWS), :])
        return 0

    lax.fori_loop(0, A_STEPS, a_step, 0)

    over_tp.wait(sums)
    sum4[...] = sumbuf4[0] + sumbuf4[1] + sumbuf4[2] + sumbuf4[3]
    over_dp = Exchange('dp', 8, sumbuf8, s8_s, s8_r)
    over_dp.start(sum4)
    sumbuf8[me] = sum4[...]

    def b_copy(b, out, core):
        at = b_at(core, b)
        return pltpu.make_async_remote_copy(
            src_ref=stage.at[out, pl.ds(0, B_ROWS), :], dst_ref=de_ref.at[pl.ds(at, B_ROWS), :],
            send_sem=b_s.at[b], recv_sem=b_r.at[b], device_id={'dp': plane.pair}, device_id_type=MESH)

    def b_free(b, slot):
        @pl.when(b >= 2)
        def _():
            keep(slot, B_ROWS, b_at(plane.core, b - 2)).wait()
            b_copy(b - 2, slot, plane.core).wait_send()

    home = pltpu.make_async_copy(dhh, dh_ref.at[pl.ds(mine, HALF), :], dh_sem)
    dh_pair = pltpu.make_async_remote_copy(
        src_ref=dhh, dst_ref=dh_ref.at[pl.ds(mine, HALF), :], send_sem=dh_s, recv_sem=dh_r,
        device_id={'tp': tp + 1 - 2 * lax.rem(tp, 2)}, device_id_type=MESH)
    dh_from_pair = pltpu.make_async_remote_copy(
        src_ref=dhh, dst_ref=dh_ref.at[pl.ds(pl.multiple_of(HALF - mine, HALF), HALF), :], send_sem=dh_s, recv_sem=dh_r,
        device_id={'tp': tp + 1 - 2 * lax.rem(tp, 2)}, device_id_type=MESH)

    def half_grad():
        far.wait()

        def part(i, _):
            at = pl.multiple_of(i * 64, 64)
            xh = xhat_ref[pl.ds(mine + at, 64), :]
            g = (dz_ref[pl.ds(at, 64), :] + far_in[pl.ds(at, 64), :]) * gamma_ref[...]
            g = g - jnp.mean(g, axis=-1, keepdims=True) - xh * jnp.mean(g * xh, axis=-1, keepdims=True)
            dhh[pl.ds(at, 64), :] = g * inv_ref[pl.ds(mine + at, 64), :]
            return 0

        lax.fori_loop(0, HALF // 64, part, 0)
        home.start()
        dh_pair.start()

    def b_step(b, _):
        slot = lax.rem(b, 2)
        at = b_at(plane.core, b)
        fetch(at, B_ROWS, slot).wait()

        @pl.when(b < B_STEPS - 2)
        def _():
            fetch(b_at(plane.core, b + 1), B_ROWS, 1 - slot).start()

        @pl.when(b == B_STEPS - 2)
        def _():
            fetch(b_at(plane.core, B_STEPS - 1), B_ROWS, 2).start()

        @pl.when(lax.rem(b, 2) == 0)
        def _():
            gather.forward(lax.div(b, 2))

        @pl.when(b == 5)
        def _():
            half_grad()

        b_free(b, slot)
        compute(slot, slot, B_ROWS, at)
        keep(slot, B_ROWS, at).start()
        b_copy(b, slot, plane.core).start()
        return 0

    lax.fori_loop(0, B_STEPS - 1, b_step, 0)

    b, slot = B_STEPS - 1, (B_STEPS - 1) % 2
    at = b_at(plane.core, b)
    fetch(at, B_ROWS, 2).wait()
    tail.wait()
    gather.forward_diag(0)
    gather.forward_diag(1)
    b_free(b, slot)
    compute(2, slot, R_MAX, at, TAIL_AT)
    keep(slot, B_ROWS, at).start()
    b_copy(b, slot, plane.core).start()
    keep_tail = pltpu.make_async_copy(stage.at[slot, pl.ds(B_ROWS, TAIL), :], de_ref.at[pl.ds(TAIL_AT, TAIL), :], t_sem)
    keep_tail.start()

    over_dp.wait(sum4)
    sums_out[...] = jnp.sum(sumbuf8[...], axis=0)
    for q in range(2, A_STEPS):
        gather.forward_diag(q)
    keep(1 - slot, B_ROWS, b_at(plane.core, b - 1)).wait()
    b_copy(b - 1, 1 - slot, plane.core).wait_send()
    keep(slot, B_ROWS, at).wait()
    keep_tail.wait()
    b_copy(b, slot, plane.core).wait_send()
    for k in range(B_STEPS):
        b_copy(k, 0, 1 - plane.core).wait_recv()
    home.wait()
    dh_pair.wait_send()
    dh_from_pair.wait_recv()
    for q in range(A_STEPS):
        keep(2 + q, A_ROWS, a_at(me, q)).wait()
        gather.own_sent(q)
        gather.finish(q)


def all_tokens(z, zall, embed, info, lse, dz, xhat, inv_std, gamma):
    return pl.pallas_call(
        all_tokens_kernel,
        name='all_tokens',
        out_shape=(
            jax.ShapeDtypeStruct((ROWS, WIDTH), F32),
            jax.ShapeDtypeStruct((SEQ, WIDTH), F32),
            jax.ShapeDtypeStruct((16, WIDTH), F32),
        ),
        in_specs=[
            pl.BlockSpec(memory_space=pltpu.VMEM),
            pl.BlockSpec(memory_space=pl.ANY),
            pl.BlockSpec(memory_space=pl.ANY),
            pl.BlockSpec(memory_space=pltpu.VMEM),
            pl.BlockSpec(memory_space=pltpu.VMEM),
            pl.BlockSpec(memory_space=pltpu.VMEM),
            pl.BlockSpec(memory_space=pltpu.VMEM),
            pl.BlockSpec(memory_space=pltpu.VMEM),
            pl.BlockSpec(memory_space=pltpu.VMEM),
        ],
        out_specs=(
            pl.BlockSpec(memory_space=pl.ANY),
            pl.BlockSpec(memory_space=pl.ANY),
            pl.BlockSpec(memory_space=pltpu.VMEM),
        ),
        scratch_shapes=[
            pltpu.VMEM((HALF, WIDTH), F32),
            pltpu.VMEM((HALF, WIDTH), F32),
            pltpu.VMEM((8, SEQ, WIDTH), BF16),
            pltpu.VMEM((4, CHUNK, WIDTH), F32),
            pltpu.VMEM((3, R_MAX + 8, WIDTH), BF16),
            pltpu.VMEM((2, R_MAX, SEQ), F32),
            pltpu.VMEM((2 + A_STEPS, R_MAX, WIDTH), F32),
            pltpu.VMEM((8, 8, SEQ), F32),
            pltpu.VMEM((8, 8, SEQ), F32),
            pltpu.VMEM((8, 8, SEQ), jnp.int32),
            pltpu.VMEM((16, WIDTH), F32),
            pltpu.VMEM((16, WIDTH), F32),
            pltpu.VMEM((4, 16, WIDTH), F32),
            pltpu.VMEM((8, 16, WIDTH), F32),
            pltpu.SemaphoreType.DMA,
            pltpu.SemaphoreType.DMA,
            pltpu.SemaphoreType.DMA,
            pltpu.SemaphoreType.DMA,
            pltpu.SemaphoreType.DMA,
            pltpu.SemaphoreType.DMA((4,)),
            pltpu.SemaphoreType.DMA((3,)),
            pltpu.SemaphoreType.DMA,
            pltpu.SemaphoreType.DMA((2 + A_STEPS,)),
            pltpu.SemaphoreType.DMA((7, A_STEPS)),
            pltpu.SemaphoreType.DMA((7, A_STEPS)),
            pltpu.SemaphoreType.DMA((B_STEPS,)),
            pltpu.SemaphoreType.DMA((B_STEPS,)),
            pltpu.SemaphoreType.DMA((4,)),
            pltpu.SemaphoreType.DMA((4,)),
            pltpu.SemaphoreType.DMA((8,)),
            pltpu.SemaphoreType.DMA((8,)),
        ],
        compiler_params=pltpu.CompilerParams(collective_id=2, has_side_effects=True, vmem_limit_bytes=60_000_000),
        cost_estimate=pl.CostEstimate(flops=32 * SEQ * 3200 * WIDTH, bytes_accessed=8 * ROWS * WIDTH, transcendentals=8 * SEQ * 3200),
    )(z, zall, embed, info, lse, dz, xhat, inv_std, gamma)


def solution(mesh):
    def local_step(hidden, ln_gamma, ln_beta, embed_shard, labels, loss_mask):
        shard_start = lax.axis_index('tp') * ROWS
        x_hat, inv_std, normed = layer_norm_fwd(hidden[0], ln_gamma, ln_beta)
        z = normed.astype(BF16)
        here = labels - shard_start
        here = jnp.where((here >= 0) & (here < ROWS), here, -1)
        info = jnp.concatenate([labels.astype(F32), loss_mask.astype(F32), here.astype(F32), jnp.zeros((5, SEQ), F32)], axis=0)
        zall, dz_half, info_all, lse_all = own_tokens(z, z.astype(F32), embed_shard, info)
        d_embed, d_rows, sums = all_tokens(z, zall, embed_shard, info_all, lse_all, dz_half, x_hat, inv_std, ln_gamma[None])
        mask = info_all[:, 1, :]
        mean_loss = jnp.sum(mask * (lse_all[:, 0, :] - lse_all[:, 1, :])) / jnp.sum(mask)
        d_gamma = jnp.sum(sums[:8], axis=0)
        d_beta = jnp.sum(sums[8:], axis=0)
        d_hidden = d_rows.astype(BF16)[None]
        return mean_loss, d_hidden, d_embed, d_gamma, d_beta

    return jax.shard_map(local_step, mesh=mesh, in_specs=(P('dp', None, None), P(None), P(None), P('tp', None), P('dp', None), P('dp', None)), out_specs=(P(), P('dp', None, None), P('tp', None), P(None), P(None)), check_vma=False)
```

```python
import jax
import jax.numpy as jnp
from jax import lax
from jax.experimental import pallas as pl
from jax.experimental.pallas import tpu as pltpu
from jax.sharding import PartitionSpec as P

LAYER_EPS = 1e-5
MESH = pl.DeviceIdType.MESH
F32, BF16 = jnp.float32, jnp.bfloat16
SEQ, WIDTH = 1024, 768
ROWS = 12568
BLOCK = 512
FULL = ROWS // BLOCK
REST = ROWS - FULL * BLOCK
RESTPAD = 384
CHUNK = 256
Z_SLOTS = 6
HALF = 512
A_ROWS, A_STEPS = 240, 4
B_ROWS, B_STEPS = 608, 4
A_TOTAL = 8 * A_ROWS * A_STEPS
TAIL = ROWS - A_TOTAL - 2 * B_ROWS * B_STEPS
TAIL_AT = ROWS - TAIL
R_MAX = B_ROWS + TAIL
VMEM_LIMIT = 67_043_328


def layer_norm_fwd(hidden, ln_gamma, ln_beta):
    x_float = hidden.astype(F32)
    row_mean = jnp.mean(x_float, axis=-1, keepdims=True)
    centered = x_float - row_mean
    inv_std = lax.rsqrt(jnp.mean(centered * centered, axis=-1, keepdims=True) + LAYER_EPS)
    x_hat = centered * inv_std
    return x_hat, inv_std, x_hat * ln_gamma + ln_beta


class Plane:
    def __init__(self):
        self.me = me = lax.axis_index('dp')
        self.core = lax.rem(me, 2)
        dx = 2 - 4 * lax.rem(lax.div(me, 2), 2)
        dy = 4 - 8 * lax.div(me, 4)
        self.x, self.y, self.diag = me + dx, me + dy, me + dx + dy
        self.pair = p = me + 1 - 2 * self.core
        self.pair_x, self.pair_y, self.pair_diag = p + dx, p + dy, p + dx + dy


class Gather:
    def __init__(self, plane, region, send_sems, recv_sems):
        self.p, self.region, self.s, self.r = plane, region, send_sems, recv_sems

    def copy(self, lane, q, src, dst, device):
        return pltpu.make_async_remote_copy(
            src_ref=src, dst_ref=dst, send_sem=self.s.at[lane, q], recv_sem=self.r.at[lane, q],
            device_id={'dp': device}, device_id_type=MESH)

    def pass_on(self, lane, q, owner, device):
        part = self.region(owner, q)
        self.copy(lane, q, part, part, device).start()

    def arrived(self, lane, q, owner):
        part = self.region(owner, q)
        self.copy(lane, q, part, part, self.p.pair).wait_recv()

    def sent(self, lane, q, owner):
        part = self.region(owner, q)
        self.copy(lane, q, part, part, self.p.pair).wait_send()

    def send_own(self, q, src):
        p = self.p
        for lane, device in ((1, p.x), (2, p.y), (0, p.pair)):
            self.copy(lane, q, src, self.region(p.me, q), device).start()

    def own_sent(self, q):
        for lane in (0, 1, 2):
            self.sent(lane, q, self.p.me)

    def forward(self, q):
        p = self.p
        self.arrived(1, q, p.x)
        self.pass_on(3, q, p.x, p.pair)

        @pl.when(lax.rem(q + p.core, 2) == 0)
        def _():
            self.pass_on(6, q, p.x, p.y)

        self.arrived(2, q, p.y)
        self.pass_on(4, q, p.y, p.pair)

        @pl.when(lax.rem(q + p.core, 2) == 1)
        def _():
            self.pass_on(6, q, p.y, p.x)

    def forward_diag(self, q):
        self.arrived(6, q, self.p.diag)
        self.pass_on(5, q, self.p.diag, self.p.pair)

    def finish(self, q):
        p = self.p
        for lane, owner in ((0, p.pair), (3, p.pair_x), (4, p.pair_y), (5, p.pair_diag)):
            self.arrived(lane, q, owner)
        for lane, owner in ((3, p.x), (4, p.y), (5, p.diag), (6, p.x)):
            self.sent(lane, q, owner)


def enter(me, tp):
    barrier = pltpu.get_barrier_semaphore()
    for o in range(1, 8):
        pl.semaphore_signal(barrier, inc=1, device_id={'dp': lax.rem(me + o, 8)}, device_id_type=MESH)
    for o in range(1, 4):
        pl.semaphore_signal(barrier, inc=1, device_id={'tp': lax.rem(tp + o, 4)}, device_id_type=MESH)
    pl.semaphore_wait(barrier, 10)


class Quarters:
    def __init__(self, tp):
        self.partner = (tp + 1 - 2 * lax.rem(tp, 2), 3 - tp)
        first, second = lax.rem(lax.div(tp + 1, 2), 2) * CHUNK, lax.div(tp, 2) * CHUNK
        self.mine = (pl.multiple_of(first, CHUNK), pl.multiple_of(HALF + second, CHUNK))
        self.theirs = (pl.multiple_of(CHUNK - first, CHUNK), pl.multiple_of(HALF + CHUNK - second, CHUNK))


class Exchange:
    def __init__(self, axis, size, buf, send_sems, recv_sems):
        self.axis, self.size, self.buf, self.s, self.r = axis, size, buf, send_sems, recv_sems
        self.me = lax.axis_index(axis)

    def copy(self, o, src, slot):
        return pltpu.make_async_remote_copy(
            src_ref=src, dst_ref=self.buf.at[slot], send_sem=self.s.at[o], recv_sem=self.r.at[o],
            device_id={self.axis: lax.rem(self.me + o, self.size)}, device_id_type=MESH)

    def start(self, src):
        for o in range(1, self.size):
            self.copy(o, src, self.me).start()

    def wait(self, src):
        for o in range(1, self.size):
            self.copy(o, src, lax.rem(self.me + self.size - o, self.size)).wait_recv()
        for o in range(1, self.size):
            self.copy(o, src, self.me).wait_send()


def offsets(groups, lanes):
    return 8 * lax.broadcasted_iota(jnp.int32, (groups, 8, lanes), 0)


def own_tokens_kernel(z_ref, zf_ref, e_ref, info_ref, zall_ref, dz_ref, info_out, lse_out,
                      logits, eslot, top, total, target, rows8, infobuf, stat, statbuf, lsend, lsebuf,
                      e_sem, half_s, half_r, zs, zr, info_s, info_r, stat_s, stat_r, lse_s, lse_r):
    plane = Plane()
    me, tp = plane.me, lax.axis_index('tp')
    enter(me, tp)

    odd = lax.rem(tp, 2)
    starts = tuple(pl.multiple_of(s, CHUNK) for s in ((2 + odd) * CHUNK, 0, CHUNK, (3 - odd) * CHUNK))

    def zregion(owner, q):
        return zall_ref.at[owner, pl.ds(starts[q], CHUNK), :]

    def across(i, owner, q):
        part = zregion(owner, q)
        return pltpu.make_async_remote_copy(
            src_ref=part, dst_ref=part, send_sem=half_s.at[i], recv_sem=half_r.at[i],
            device_id={'tp': tp + 1 - 2 * odd}, device_id_type=MESH)

    gather = Gather(plane, zregion, zs, zr)
    infos = Exchange('dp', 8, infobuf, info_s, info_r)
    infos.start(info_ref)
    own = tuple(zf_ref.at[pl.ds(s, CHUNK), :] for s in starts)
    gather.send_own(0, own[0])
    gather.copy(0, 3, own[3], zregion(me, 3), plane.pair).start()
    infobuf[me] = info_ref[...]

    def fetch(j, slot):
        return pltpu.make_async_copy(
            e_ref.at[pl.ds(pl.multiple_of(j * BLOCK, BLOCK), BLOCK), :], eslot.at[slot], e_sem.at[slot])

    def fetch_rest(slot):
        return pltpu.make_async_copy(
            e_ref.at[pl.ds(FULL * BLOCK, REST), :], eslot.at[slot, pl.ds(0, REST), :], e_sem.at[slot])

    def blocks(body, hooks):
        fetch(0, 0).start()

        def step(j, _):
            slot = lax.rem(j, 2)
            fetch(j, slot).wait()

            @pl.when(j < FULL - 1)
            def _():
                fetch(j + 1, 1 - slot).start()

            @pl.when(j == FULL - 1)
            def _():
                eslot[1 - slot, pl.ds(272, RESTPAD - 272), :] = jnp.zeros((RESTPAD - 272, WIDTH), BF16)
                fetch_rest(1 - slot).start()

            for at, hook in hooks:
                pl.when(j == at)(hook)
            body(pl.multiple_of(j * BLOCK, BLOCK), slot, BLOCK)
            return 0

        lax.fori_loop(0, FULL, step, 0)
        fetch_rest(FULL % 2).wait()
        body(FULL * BLOCK, FULL % 2, RESTPAD)

    sub = lax.broadcasted_iota(jnp.int32, (8, SEQ), 0)
    rows8[0] = jnp.broadcast_to(info_ref[2:3, :].astype(jnp.int32), (8, SEQ)) - sub
    top[...] = jnp.full((8, SEQ), -jnp.inf, F32)
    total[...] = jnp.zeros((8, SEQ), F32)
    target[...] = jnp.zeros((8, SEQ), F32)

    def forward_block(at, slot, n):
        e = eslot[slot, pl.ds(0, n), :]
        for t in range(4):
            cols = pl.ds(t * CHUNK, CHUNK)
            l = lax.dot_general(e, z_ref[cols, :], (((1,), (1,)), ((), ())), preferred_element_type=F32)
            if n != BLOCK:
                l = jnp.where(lax.broadcasted_iota(jnp.int32, (n, CHUNK), 0) < REST, l, -jnp.inf)
            logits[pl.ds(at, n), cols] = l
            l = l.reshape(n // 8, 8, CHUNK)
            old = top[:, cols]
            new = jnp.maximum(old, jnp.max(l, axis=0))
            top[:, cols] = new
            total[:, cols] = total[:, cols] * jnp.exp(old - new) + jnp.sum(jnp.exp(l - new[None]), axis=0)
            hit = offsets(n // 8, CHUNK) == (rows8[0, :, cols] - at)[None]
            target[:, cols] += jnp.sum(jnp.where(hit, l, 0.0), axis=0)

    def first_chunk():
        gather.forward(0)
        across(0, plane.x, 0).start()
        gather.send_own(1, own[1])
        gather.send_own(2, own[2])

    blocks(forward_block, ((12, first_chunk),))

    m1 = jnp.max(top[...], axis=0, keepdims=True)
    stat[0:1, :] = m1
    stat[1:2, :] = jnp.sum(total[...] * jnp.exp(top[...] - m1), axis=0, keepdims=True)
    stat[2:3, :] = jnp.sum(target[...], axis=0, keepdims=True)
    stats = Exchange('tp', 4, statbuf, stat_s, stat_r)
    stats.start(stat)
    statbuf[tp] = stat[...]
    infos.wait(info_ref)
    token_count = jnp.sum(infobuf[:, 1, :], keepdims=True)
    stats.wait(stat)
    m4 = jnp.max(statbuf[:, 0, :], axis=0, keepdims=True)
    s4 = jnp.sum(statbuf[:, 1, :] * jnp.exp(statbuf[:, 0, :] - m4), axis=0, keepdims=True)
    lse = m4 + jnp.log(s4)
    lsend[0:1, :] = lse
    lsend[1:2, :] = jnp.sum(statbuf[:, 2, :], axis=0, keepdims=True)
    lses = Exchange('dp', 8, lsebuf, lse_s, lse_r)
    lses.start(lsend)
    lsebuf[me] = lsend[...]
    top[...] = jnp.broadcast_to(lse, (8, SEQ))
    total[...] = jnp.broadcast_to(info_ref[1:2, :] / token_count, (8, SEQ))
    across(1, plane.y, 0).start()
    gather.forward_diag(0)
    across(2, plane.diag, 0).start()

    dz_ref[...] = jnp.zeros((SEQ, WIDTH), F32)

    def backward_block(at, slot, n):
        e = eslot[slot, pl.ds(0, n), :]
        for t in range(4):
            cols = pl.ds(t * CHUNK, CHUNK)
            l = logits[pl.ds(at, n), cols].reshape(n // 8, 8, CHUNK)
            p = jnp.exp(l - top[:, cols][None])
            hit = offsets(n // 8, CHUNK) == (rows8[0, :, cols] - at)[None]
            g = (jnp.where(hit, p - 1.0, p) * total[:, cols][None]).reshape(n, CHUNK).astype(BF16)
            dz_ref[cols, :] += lax.dot_general(g, e, (((0,), (0,)), ((), ())), preferred_element_type=F32)

    blocks(backward_block, ((8, lambda: gather.forward(1)), (18, lambda: gather.forward(2))))

    for i, (lane, owner) in enumerate(((3, plane.x), (4, plane.y), (5, plane.diag))):
        across(i, owner, 3).wait_recv()
        gather.pass_on(lane, 3, owner, plane.pair)
    lses.wait(lsend)
    info_out[...] = infobuf[...]
    lse_out[...] = lsebuf[...]
    for q in (1, 2):
        gather.forward_diag(q)
    for q in range(3):
        gather.own_sent(q)
        gather.finish(q)
    gather.sent(0, 3, me)
    for lane, owner in ((0, plane.pair), (3, plane.pair_x), (4, plane.pair_y), (5, plane.pair_diag)):
        gather.arrived(lane, 3, owner)
    for i, (lane, owner) in enumerate(((3, plane.x), (4, plane.y), (5, plane.diag))):
        gather.sent(lane, 3, owner)
        across(i, owner, 0).wait_send()


def own_tokens(z, zf, embed, info):
    return pl.pallas_call(
        own_tokens_kernel,
        name='own_tokens',
        out_shape=(
            jax.ShapeDtypeStruct((8, SEQ, WIDTH), F32),
            jax.ShapeDtypeStruct((SEQ, WIDTH), F32),
            jax.ShapeDtypeStruct((8, 8, SEQ), F32),
            jax.ShapeDtypeStruct((8, 8, SEQ), F32),
        ),
        in_specs=[
            pl.BlockSpec(memory_space=pltpu.VMEM),
            pl.BlockSpec(memory_space=pl.ANY),
            pl.BlockSpec(memory_space=pl.ANY),
            pl.BlockSpec(memory_space=pltpu.VMEM),
        ],
        out_specs=(
            pl.BlockSpec(memory_space=pl.ANY),
            pl.BlockSpec(memory_space=pltpu.VMEM),
            pl.BlockSpec(memory_space=pltpu.VMEM),
            pl.BlockSpec(memory_space=pltpu.VMEM),
        ),
        scratch_shapes=[
            pltpu.VMEM((FULL * BLOCK + RESTPAD, SEQ), F32),
            pltpu.VMEM((2, BLOCK, WIDTH), BF16),
            pltpu.VMEM((8, SEQ), F32),
            pltpu.VMEM((8, SEQ), F32),
            pltpu.VMEM((8, SEQ), F32),
            pltpu.VMEM((1, 8, SEQ), jnp.int32),
            pltpu.VMEM((8, 8, SEQ), F32),
            pltpu.VMEM((8, SEQ), F32),
            pltpu.VMEM((4, 8, SEQ), F32),
            pltpu.VMEM((8, SEQ), F32),
            pltpu.VMEM((8, 8, SEQ), F32),
            pltpu.SemaphoreType.DMA((2,)),
            pltpu.SemaphoreType.DMA((3,)),
            pltpu.SemaphoreType.DMA((3,)),
            pltpu.SemaphoreType.DMA((7, 4)),
            pltpu.SemaphoreType.DMA((7, 4)),
            pltpu.SemaphoreType.DMA((8,)),
            pltpu.SemaphoreType.DMA((8,)),
            pltpu.SemaphoreType.DMA((4,)),
            pltpu.SemaphoreType.DMA((4,)),
            pltpu.SemaphoreType.DMA((8,)),
            pltpu.SemaphoreType.DMA((8,)),
        ],
        compiler_params=pltpu.CompilerParams(collective_id=1, has_side_effects=True, vmem_limit_bytes=VMEM_LIMIT),
        cost_estimate=pl.CostEstimate(flops=4 * SEQ * ROWS * WIDTH, bytes_accessed=4 * ROWS * WIDTH, transcendentals=2 * SEQ * ROWS),
    )(z, zf, embed, info)


def all_tokens_kernel(z_ref, zall_ref, e_ref, info_ref, lse_ref, dzp_ref, xhat_ref, inv_ref, gamma_ref, de_ref, dh_ref, sums_out,
                      half_in, dzh, far_in, dhh, zb, zslot, eslot, lbuf, stage_a, stage_b, lse8, scale8, rows8, sums, sum4, sumbuf4, sumbuf8,
                      half_s, half_r, far_s, far_r, dh_sem, dh_s, dh_r, z_sem, e_sem, t_sem, l_sem, gs, gr, b_s, b_r, s4_s, s4_r, s8_s, s8_r):
    plane = Plane()
    me, tp = plane.me, lax.axis_index('tp')
    enter(me, tp)

    def fetch(at, n, slot):
        return pltpu.make_async_copy(e_ref.at[pl.ds(at, n), :], eslot.at[slot, pl.ds(0, n), :], e_sem.at[slot])

    def a_at(owner, q):
        return pl.multiple_of((owner * A_STEPS + q) * A_ROWS, 16)

    def b_at(core, b):
        return pl.multiple_of(A_TOTAL + (core * B_STEPS + b) * B_ROWS, 16)

    fetch(a_at(me, 0), A_ROWS, 0).start()
    tail = pltpu.make_async_copy(e_ref.at[pl.ds(TAIL_AT, TAIL), :], eslot.at[2, pl.ds(B_ROWS, TAIL), :], t_sem)
    tail.start()

    quarters = Quarters(tp)

    def swap_with(k, partner, src, dst, send_sem, recv_sem):
        return pltpu.make_async_remote_copy(
            src_ref=src, dst_ref=dst.at[k], send_sem=send_sem.at[k], recv_sem=recv_sem.at[k],
            device_id={'tp': partner}, device_id_type=MESH)

    nears = [swap_with(k, quarters.partner[k], dzp_ref.at[pl.ds(quarters.theirs[k], CHUNK), :], half_in, half_s, half_r) for k in range(2)]
    fars = [swap_with(k, quarters.partner[1 - k], dzh.at[k], far_in, far_s, far_r) for k in range(2)]
    for near in nears:
        near.start()

    def fetch_z(n):
        owner = lax.rem(me + 1 + lax.div(n, 4), 8)
        q = pl.multiple_of(lax.rem(n, 4) * CHUNK, CHUNK)
        slot = lax.rem(n, Z_SLOTS)
        return owner, q, slot, pltpu.make_async_copy(zall_ref.at[owner, pl.ds(q, CHUNK), :], zslot.at[slot], z_sem.at[slot])

    for n in range(Z_SLOTS - 1):
        fetch_z(n)[3].start()
    zb[me] = z_ref[...]
    token_count = jnp.sum(info_ref[:, 1, :], keepdims=True)
    sub = lax.broadcasted_iota(jnp.int32, (8, SEQ), 0) + tp * ROWS
    for s in range(8):
        lse8[s] = jnp.broadcast_to(lse_ref[s, 0:1, :], (8, SEQ))
        scale8[s] = jnp.broadcast_to(info_ref[s, 1:2, :] / token_count, (8, SEQ))
        rows8[s] = jnp.broadcast_to(info_ref[s, 0:1, :].astype(jnp.int32), (8, SEQ)) - sub

    def convert(n, _):
        owner, q, slot, copy = fetch_z(n)
        copy.wait()

        @pl.when(n < 29 - Z_SLOTS)
        def _():
            fetch_z(n + Z_SLOTS - 1)[3].start()

        zb[owner, pl.ds(q, CHUNK), :] = zslot[slot].astype(BF16)
        return 0

    def logits_of(slot, n, s):
        return lax.dot_general(eslot[slot, pl.ds(0, n), :], zb[s], (((1,), (1,)), ((), ())), preferred_element_type=F32)

    def grad_of(l, n, s, at, tail_at):
        l = l.reshape(n // 8, 8, SEQ)
        p = jnp.exp(l - lse8[s][None])
        row = offsets(n // 8, SEQ) + at
        if tail_at is not None:
            row = jnp.where(offsets(n // 8, SEQ) < B_ROWS, row, row + (tail_at - B_ROWS - at))
        g = jnp.where(row == rows8[s][None], p - 1.0, p) * scale8[s][None]
        return g.reshape(n, SEQ).astype(BF16)

    def compute(slot, out, n, at, tail_at=None, arriving=False):
        lbuf[0, pl.ds(0, n), :] = logits_of(slot, n, me)
        out[...] = jnp.zeros((n, WIDTH), F32)

        def one(i, k, last):
            s = lax.rem(me + i, 8)
            if not last:
                if arriving:
                    lax.fori_loop(4 * i, 4 * i + 4, convert, 0)
                lbuf[1 - k, pl.ds(0, n), :] = logits_of(slot, n, lax.rem(me + i + 1, 8))
            g = grad_of(lbuf[k, pl.ds(0, n), :], n, s, at, tail_at)
            out[...] += jnp.dot(g, zb[s], preferred_element_type=F32)

        def pairs(i, _):
            one(2 * i, 0, False)
            one(2 * i + 1, 1, False)
            return 0

        lax.fori_loop(0, 3, pairs, 0)
        one(6, 0, False)
        one(7, 1, True)

    def region(owner, q):
        return de_ref.at[pl.ds(a_at(owner, q), A_ROWS), :]

    gather = Gather(plane, region, gs, gr)

    def keep(k, n, at):
        out = stage_a.at[k] if n == A_ROWS else stage_b.at[k - A_STEPS, pl.ds(0, n), :]
        return pltpu.make_async_copy(out, de_ref.at[pl.ds(at, n), :], l_sem.at[k])

    over_tp = Exchange('tp', 4, sumbuf4, s4_s, s4_r)

    def near_sums():
        dgamma = dbeta = jnp.zeros((8, WIDTH), F32)
        for k in range(2):
            nears[k].wait()

            def part(i, carry):
                at = pl.multiple_of(i * 64, 64)
                rows = pl.ds(pl.multiple_of(quarters.mine[k] + at, 64), 64)
                dz = dzp_ref[rows, :] + half_in[k, pl.ds(at, 64), :]
                dzh[k, pl.ds(at, 64), :] = dz
                dzx = dz * xhat_ref[rows, :]
                return carry[0] + jnp.sum(dzx.reshape(8, 8, WIDTH), axis=0), carry[1] + jnp.sum(dz.reshape(8, 8, WIDTH), axis=0)

            dgamma, dbeta = lax.fori_loop(0, CHUNK // 64, part, (dgamma, dbeta))
        sums[0:8, :] = dgamma
        sums[8:16, :] = dbeta
        over_tp.start(sums)
        for far in fars:
            far.start()
        sumbuf4[tp] = sums[...]

    def home(k):
        return pltpu.make_async_copy(dhh.at[k], dh_ref.at[pl.ds(quarters.mine[k], CHUNK), :], dh_sem.at[k])

    def swap_rows(k, rows):
        return pltpu.make_async_remote_copy(
            src_ref=dhh.at[k], dst_ref=dh_ref.at[pl.ds(rows, CHUNK), :], send_sem=dh_s.at[k], recv_sem=dh_r.at[k],
            device_id={'tp': quarters.partner[k]}, device_id_type=MESH)

    over_dp = Exchange('dp', 8, sumbuf8, s8_s, s8_r)

    def far_grads():
        over_tp.wait(sums)
        sum4[...] = sumbuf4[0] + sumbuf4[1] + sumbuf4[2] + sumbuf4[3]
        over_dp.start(sum4)
        sumbuf8[me] = sum4[...]
        for k in range(2):
            fars[k].wait()

            def part(i, _):
                at = pl.multiple_of(i * 64, 64)
                rows = pl.ds(pl.multiple_of(quarters.mine[k] + at, 64), 64)
                xh = xhat_ref[rows, :]
                g = (dzh[k, pl.ds(at, 64), :] + far_in[k, pl.ds(at, 64), :]) * gamma_ref[...]
                g = g - jnp.mean(g, axis=-1, keepdims=True) - xh * jnp.mean(g * xh, axis=-1, keepdims=True)
                dhh[k, pl.ds(at, 64), :] = g * inv_ref[rows, :]
                return 0

            lax.fori_loop(0, CHUNK // 64, part, 0)
            home(k).start()
            swap_rows(k, quarters.mine[k]).start()

    def a_step(q, _, first=False):
        slot = lax.rem(q, 2)
        fetch(a_at(me, q), A_ROWS, slot).wait()

        @pl.when(q < A_STEPS - 1)
        def _():
            fetch(a_at(me, q + 1), A_ROWS, 1 - slot).start()

        @pl.when(q == A_STEPS - 1)
        def _():
            fetch(b_at(plane.core, 0), B_ROWS, 1 - slot).start()

        if not first:
            pl.when(q == A_STEPS - 1)(near_sums)
        if first:
            compute(slot, stage_a.at[q], A_ROWS, a_at(me, q), arriving=True)
        else:
            compute(slot, stage_a.at[q], A_ROWS, a_at(me, q))
        keep(q, A_ROWS, a_at(me, q)).start()
        gather.send_own(q, stage_a.at[q])
        return 0

    a_step(0, 0, first=True)
    lax.fori_loop(1, A_STEPS, a_step, 0)

    def b_copy(b, out, core):
        at = b_at(core, b)
        return pltpu.make_async_remote_copy(
            src_ref=stage_b.at[out - A_STEPS, pl.ds(0, B_ROWS), :], dst_ref=de_ref.at[pl.ds(at, B_ROWS), :],
            send_sem=b_s.at[b], recv_sem=b_r.at[b], device_id={'dp': plane.pair}, device_id_type=MESH)

    def b_step(b, _):
        slot = lax.rem(b, 2)
        at = b_at(plane.core, b)
        fetch(at, B_ROWS, slot).wait()

        @pl.when(b < B_STEPS - 2)
        def _():
            fetch(b_at(plane.core, b + 1), B_ROWS, 1 - slot).start()

        @pl.when(b == B_STEPS - 2)
        def _():
            fetch(b_at(plane.core, B_STEPS - 1), B_ROWS, 2).start()

        @pl.when(lax.rem(b, B_STEPS // 4) == 0)
        def _():
            gather.forward(lax.div(b, B_STEPS // 4))

        pl.when(b == B_STEPS // 2)(far_grads)
        compute(slot, stage_b.at[b, pl.ds(0, B_ROWS), :], B_ROWS, at)
        keep(A_STEPS + b, B_ROWS, at).start()
        b_copy(b, A_STEPS + b, plane.core).start()
        return 0

    lax.fori_loop(0, B_STEPS - 1, b_step, 0)

    b, slot = B_STEPS - 1, A_STEPS + B_STEPS - 1
    at = b_at(plane.core, b)
    fetch(at, B_ROWS, 2).wait()
    tail.wait()
    if B_STEPS == 4:
        gather.forward(3)
    gather.forward_diag(0)
    gather.forward_diag(1)
    compute(2, stage_b.at[b], R_MAX, at, TAIL_AT)
    keep(slot, B_ROWS, at).start()
    b_copy(b, slot, plane.core).start()
    keep_tail = pltpu.make_async_copy(stage_b.at[b, pl.ds(B_ROWS, TAIL), :], de_ref.at[pl.ds(TAIL_AT, TAIL), :], t_sem)
    keep_tail.start()

    over_dp.wait(sum4)
    sums_out[...] = jnp.sum(sumbuf8[...], axis=0)
    for q in range(2, A_STEPS):
        gather.forward_diag(q)
    keep_tail.wait()
    for k in range(B_STEPS):
        keep(A_STEPS + k, B_ROWS, b_at(plane.core, k)).wait()
        b_copy(k, A_STEPS + k, plane.core).wait_send()
        b_copy(k, A_STEPS + k, 1 - plane.core).wait_recv()
    for k in range(2):
        home(k).wait()
        swap_rows(k, quarters.mine[k]).wait_send()
        swap_rows(k, quarters.theirs[k]).wait_recv()
    for q in range(A_STEPS):
        keep(q, A_ROWS, a_at(me, q)).wait()
        gather.own_sent(q)
        gather.finish(q)


def all_tokens(z, zall, embed, info, lse, dz, xhat, inv_std, gamma):
    return pl.pallas_call(
        all_tokens_kernel,
        name='all_tokens',
        out_shape=(
            jax.ShapeDtypeStruct((ROWS, WIDTH), F32),
            jax.ShapeDtypeStruct((SEQ, WIDTH), F32),
            jax.ShapeDtypeStruct((16, WIDTH), F32),
        ),
        in_specs=[
            pl.BlockSpec(memory_space=pltpu.VMEM),
            pl.BlockSpec(memory_space=pl.ANY),
            pl.BlockSpec(memory_space=pl.ANY),
            pl.BlockSpec(memory_space=pltpu.VMEM),
            pl.BlockSpec(memory_space=pltpu.VMEM),
            pl.BlockSpec(memory_space=pltpu.VMEM),
            pl.BlockSpec(memory_space=pltpu.VMEM),
            pl.BlockSpec(memory_space=pltpu.VMEM),
            pl.BlockSpec(memory_space=pltpu.VMEM),
        ],
        out_specs=(
            pl.BlockSpec(memory_space=pl.ANY),
            pl.BlockSpec(memory_space=pl.ANY),
            pl.BlockSpec(memory_space=pltpu.VMEM),
        ),
        scratch_shapes=[
            pltpu.VMEM((2, CHUNK, WIDTH), F32),
            pltpu.VMEM((2, CHUNK, WIDTH), F32),
            pltpu.VMEM((2, CHUNK, WIDTH), F32),
            pltpu.VMEM((2, CHUNK, WIDTH), F32),
            pltpu.VMEM((8, SEQ, WIDTH), BF16),
            pltpu.VMEM((Z_SLOTS, CHUNK, WIDTH), F32),
            pltpu.VMEM((3, R_MAX + 8, WIDTH), BF16),
            pltpu.VMEM((2, R_MAX, SEQ), F32),
            pltpu.VMEM((A_STEPS, A_ROWS, WIDTH), F32),
            pltpu.VMEM((B_STEPS, R_MAX, WIDTH), F32),
            pltpu.VMEM((8, 8, SEQ), F32),
            pltpu.VMEM((8, 8, SEQ), F32),
            pltpu.VMEM((8, 8, SEQ), jnp.int32),
            pltpu.VMEM((16, WIDTH), F32),
            pltpu.VMEM((16, WIDTH), F32),
            pltpu.VMEM((4, 16, WIDTH), F32),
            pltpu.VMEM((8, 16, WIDTH), F32),
            pltpu.SemaphoreType.DMA((2,)),
            pltpu.SemaphoreType.DMA((2,)),
            pltpu.SemaphoreType.DMA((2,)),
            pltpu.SemaphoreType.DMA((2,)),
            pltpu.SemaphoreType.DMA((2,)),
            pltpu.SemaphoreType.DMA((2,)),
            pltpu.SemaphoreType.DMA((2,)),
            pltpu.SemaphoreType.DMA((Z_SLOTS,)),
            pltpu.SemaphoreType.DMA((3,)),
            pltpu.SemaphoreType.DMA,
            pltpu.SemaphoreType.DMA((A_STEPS + B_STEPS,)),
            pltpu.SemaphoreType.DMA((7, A_STEPS)),
            pltpu.SemaphoreType.DMA((7, A_STEPS)),
            pltpu.SemaphoreType.DMA((B_STEPS,)),
            pltpu.SemaphoreType.DMA((B_STEPS,)),
            pltpu.SemaphoreType.DMA((4,)),
            pltpu.SemaphoreType.DMA((4,)),
            pltpu.SemaphoreType.DMA((8,)),
            pltpu.SemaphoreType.DMA((8,)),
        ],
        compiler_params=pltpu.CompilerParams(collective_id=2, has_side_effects=True, vmem_limit_bytes=VMEM_LIMIT),
        cost_estimate=pl.CostEstimate(flops=32 * SEQ * 3200 * WIDTH, bytes_accessed=8 * ROWS * WIDTH, transcendentals=8 * SEQ * 3200),
    )(z, zall, embed, info, lse, dz, xhat, inv_std, gamma)


def solution(mesh):
    def local_step(hidden, ln_gamma, ln_beta, embed_shard, labels, loss_mask):
        shard_start = lax.axis_index('tp') * ROWS
        x_hat, inv_std, normed = layer_norm_fwd(hidden[0], ln_gamma, ln_beta)
        z = normed.astype(BF16)
        here = labels - shard_start
        here = jnp.where((here >= 0) & (here < ROWS), here, -1)
        info = jnp.concatenate([labels.astype(F32), loss_mask.astype(F32), here.astype(F32), jnp.zeros((5, SEQ), F32)], axis=0)
        zall, dz_part, info_all, lse_all = own_tokens(z, z.astype(F32), embed_shard, info)
        d_embed, d_rows, sums = all_tokens(z, zall, embed_shard, info_all, lse_all, dz_part, x_hat, inv_std, ln_gamma[None])
        mask = info_all[:, 1, :]
        mean_loss = jnp.sum(mask * (lse_all[:, 0, :] - lse_all[:, 1, :])) / jnp.sum(mask)
        d_gamma = jnp.sum(sums[:8], axis=0)
        d_beta = jnp.sum(sums[8:], axis=0)
        d_hidden = d_rows.astype(BF16)[None]
        return mean_loss, d_hidden, d_embed, d_gamma, d_beta

    return jax.shard_map(local_step, mesh=mesh, in_specs=(P('dp', None, None), P(None), P(None), P('tp', None), P('dp', None), P('dp', None)), out_specs=(P(), P('dp', None, None), P('tp', None), P(None), P(None)), check_vma=False)
```

```python
import jax
import jax.numpy as jnp
from jax import lax
from jax.experimental import pallas as pl
from jax.experimental.pallas import tpu as pltpu
from jax.sharding import PartitionSpec as P

LAYER_EPS = 1e-5
MESH = pl.DeviceIdType.MESH
F32, BF16 = jnp.float32, jnp.bfloat16
SEQ, WIDTH = 1024, 768
ROWS = 12568
BLOCK = 512
FULL = ROWS // BLOCK
REST = ROWS - FULL * BLOCK
RESTPAD = 384
CHUNK = 256
Z_SLOTS = 6
HALF = 512
A_ROWS, A_STEPS = 240, 4
B_ROWS, B_STEPS = 608, 4
A_TOTAL = 8 * A_ROWS * A_STEPS
TAIL = ROWS - A_TOTAL - 2 * B_ROWS * B_STEPS
TAIL_AT = ROWS - TAIL
R_MAX = B_ROWS + TAIL
VMEM_LIMIT = 67_043_328


def layer_norm_fwd(hidden, ln_gamma, ln_beta):
    x_float = hidden.astype(F32)
    row_mean = jnp.mean(x_float, axis=-1, keepdims=True)
    centered = x_float - row_mean
    inv_std = lax.rsqrt(jnp.mean(centered * centered, axis=-1, keepdims=True) + LAYER_EPS)
    x_hat = centered * inv_std
    return x_hat, inv_std, x_hat * ln_gamma + ln_beta


class Plane:
    def __init__(self):
        self.me = me = lax.axis_index('dp')
        self.core = lax.rem(me, 2)
        dx = 2 - 4 * lax.rem(lax.div(me, 2), 2)
        dy = 4 - 8 * lax.div(me, 4)
        self.x, self.y, self.diag = me + dx, me + dy, me + dx + dy
        self.pair = p = me + 1 - 2 * self.core
        self.pair_x, self.pair_y, self.pair_diag = p + dx, p + dy, p + dx + dy


class Gather:
    def __init__(self, plane, region, send_sems, recv_sems):
        self.p, self.region, self.s, self.r = plane, region, send_sems, recv_sems

    def copy(self, lane, q, src, dst, device):
        return pltpu.make_async_remote_copy(
            src_ref=src, dst_ref=dst, send_sem=self.s.at[lane, q], recv_sem=self.r.at[lane, q],
            device_id={'dp': device}, device_id_type=MESH)

    def pass_on(self, lane, q, owner, device):
        part = self.region(owner, q)
        self.copy(lane, q, part, part, device).start()

    def arrived(self, lane, q, owner):
        part = self.region(owner, q)
        self.copy(lane, q, part, part, self.p.pair).wait_recv()

    def sent(self, lane, q, owner):
        part = self.region(owner, q)
        self.copy(lane, q, part, part, self.p.pair).wait_send()

    def send_own(self, q, src):
        p = self.p
        for lane, device in ((1, p.x), (2, p.y), (0, p.pair)):
            self.copy(lane, q, src, self.region(p.me, q), device).start()

    def own_sent(self, q):
        for lane in (0, 1, 2):
            self.sent(lane, q, self.p.me)

    def forward(self, q):
        p = self.p
        self.arrived(1, q, p.x)
        self.pass_on(3, q, p.x, p.pair)

        @pl.when(lax.rem(q + p.core, 2) == 0)
        def _():
            self.pass_on(6, q, p.x, p.y)

        self.arrived(2, q, p.y)
        self.pass_on(4, q, p.y, p.pair)

        @pl.when(lax.rem(q + p.core, 2) == 1)
        def _():
            self.pass_on(6, q, p.y, p.x)

    def forward_diag(self, q):
        self.arrived(6, q, self.p.diag)
        self.pass_on(5, q, self.p.diag, self.p.pair)

    def finish(self, q):
        p = self.p
        for lane, owner in ((0, p.pair), (3, p.pair_x), (4, p.pair_y), (5, p.pair_diag)):
            self.arrived(lane, q, owner)
        for lane, owner in ((3, p.x), (4, p.y), (5, p.diag), (6, p.x)):
            self.sent(lane, q, owner)


def enter(me, tp):
    barrier = pltpu.get_barrier_semaphore()
    for o in range(1, 8):
        pl.semaphore_signal(barrier, inc=1, device_id={'dp': lax.rem(me + o, 8)}, device_id_type=MESH)
    for o in range(1, 4):
        pl.semaphore_signal(barrier, inc=1, device_id={'tp': lax.rem(tp + o, 4)}, device_id_type=MESH)
    pl.semaphore_wait(barrier, 10)


class Quarters:
    def __init__(self, tp):
        self.partner = (tp + 1 - 2 * lax.rem(tp, 2), 3 - tp)
        first, second = lax.rem(lax.div(tp + 1, 2), 2) * CHUNK, lax.div(tp, 2) * CHUNK
        self.mine = (pl.multiple_of(first, CHUNK), pl.multiple_of(HALF + second, CHUNK))
        self.theirs = (pl.multiple_of(CHUNK - first, CHUNK), pl.multiple_of(HALF + CHUNK - second, CHUNK))


class Exchange:
    def __init__(self, axis, size, buf, send_sems, recv_sems):
        self.axis, self.size, self.buf, self.s, self.r = axis, size, buf, send_sems, recv_sems
        self.me = lax.axis_index(axis)

    def copy(self, o, src, slot):
        return pltpu.make_async_remote_copy(
            src_ref=src, dst_ref=self.buf.at[slot], send_sem=self.s.at[o], recv_sem=self.r.at[o],
            device_id={self.axis: lax.rem(self.me + o, self.size)}, device_id_type=MESH)

    def start(self, src):
        for o in range(1, self.size):
            self.copy(o, src, self.me).start()

    def wait(self, src):
        for o in range(1, self.size):
            self.copy(o, src, lax.rem(self.me + self.size - o, self.size)).wait_recv()
        for o in range(1, self.size):
            self.copy(o, src, self.me).wait_send()


def offsets(groups, lanes):
    return 8 * lax.broadcasted_iota(jnp.int32, (groups, 8, lanes), 0)


def own_tokens_kernel(z_ref, zf_ref, e_ref, info_ref, zall_ref, dz_ref, info_out, lse_out,
                      logits, eslot, top, total, target, rows8, infobuf, stat, statbuf, lsend, lsebuf,
                      e_sem, half_s, half_r, zs, zr, info_s, info_r, stat_s, stat_r, lse_s, lse_r):
    plane = Plane()
    me, tp = plane.me, lax.axis_index('tp')
    enter(me, tp)

    odd = lax.rem(tp, 2)
    starts = tuple(pl.multiple_of(s, CHUNK) for s in ((2 + odd) * CHUNK, 0, CHUNK, (3 - odd) * CHUNK))

    def zregion(owner, q):
        return zall_ref.at[owner, pl.ds(starts[q], CHUNK), :]

    def across(i, owner, q):
        part = zregion(owner, q)
        return pltpu.make_async_remote_copy(
            src_ref=part, dst_ref=part, send_sem=half_s.at[i], recv_sem=half_r.at[i],
            device_id={'tp': tp + 1 - 2 * odd}, device_id_type=MESH)

    gather = Gather(plane, zregion, zs, zr)
    infos = Exchange('dp', 8, infobuf, info_s, info_r)
    infos.start(info_ref)
    own = tuple(zf_ref.at[pl.ds(s, CHUNK), :] for s in starts)
    gather.send_own(0, own[0])
    gather.copy(0, 3, own[3], zregion(me, 3), plane.pair).start()
    infobuf[me] = info_ref[...]

    def fetch(j, slot):
        return pltpu.make_async_copy(
            e_ref.at[pl.ds(pl.multiple_of(j * BLOCK, BLOCK), BLOCK), :], eslot.at[slot], e_sem.at[slot])

    def fetch_rest(slot):
        return pltpu.make_async_copy(
            e_ref.at[pl.ds(FULL * BLOCK, REST), :], eslot.at[slot, pl.ds(0, REST), :], e_sem.at[slot])

    def blocks(body, hooks):
        fetch(0, 0).start()

        def step(j, _):
            slot = lax.rem(j, 2)
            fetch(j, slot).wait()

            @pl.when(j < FULL - 1)
            def _():
                fetch(j + 1, 1 - slot).start()

            @pl.when(j == FULL - 1)
            def _():
                eslot[1 - slot, pl.ds(272, RESTPAD - 272), :] = jnp.zeros((RESTPAD - 272, WIDTH), BF16)
                fetch_rest(1 - slot).start()

            for at, hook in hooks:
                pl.when(j == at)(hook)
            body(pl.multiple_of(j * BLOCK, BLOCK), slot, BLOCK)
            return 0

        lax.fori_loop(0, FULL, step, 0)
        fetch_rest(FULL % 2).wait()
        body(FULL * BLOCK, FULL % 2, RESTPAD)

    sub = lax.broadcasted_iota(jnp.int32, (8, SEQ), 0)
    rows8[0] = jnp.broadcast_to(info_ref[2:3, :].astype(jnp.int32), (8, SEQ)) - sub
    top[...] = jnp.full((8, SEQ), -jnp.inf, F32)
    total[...] = jnp.zeros((8, SEQ), F32)
    target[...] = jnp.zeros((8, SEQ), F32)

    def forward_block(at, slot, n):
        e = eslot[slot, pl.ds(0, n), :]
        for t in range(4):
            cols = pl.ds(t * CHUNK, CHUNK)
            l = lax.dot_general(e, z_ref[cols, :], (((1,), (1,)), ((), ())), preferred_element_type=F32)
            if n != BLOCK:
                l = jnp.where(lax.broadcasted_iota(jnp.int32, (n, CHUNK), 0) < REST, l, -jnp.inf)
            logits[pl.ds(at, n), cols] = l
            l = l.reshape(n // 8, 8, CHUNK)
            old = top[:, cols]
            new = jnp.maximum(old, jnp.max(l, axis=0))
            top[:, cols] = new
            total[:, cols] = total[:, cols] * jnp.exp(old - new) + jnp.sum(jnp.exp(l - new[None]), axis=0)
            hit = offsets(n // 8, CHUNK) == (rows8[0, :, cols] - at)[None]
            target[:, cols] += jnp.sum(jnp.where(hit, l, 0.0), axis=0)

    def first_chunk():
        gather.forward(0)
        across(0, plane.x, 0).start()
        gather.send_own(1, own[1])
        gather.send_own(2, own[2])

    blocks(forward_block, ((12, first_chunk),))

    m1 = jnp.max(top[...], axis=0, keepdims=True)
    stat[0:1, :] = m1
    stat[1:2, :] = jnp.sum(total[...] * jnp.exp(top[...] - m1), axis=0, keepdims=True)
    stat[2:3, :] = jnp.sum(target[...], axis=0, keepdims=True)
    stats = Exchange('tp', 4, statbuf, stat_s, stat_r)
    stats.start(stat)
    statbuf[tp] = stat[...]
    infos.wait(info_ref)
    token_count = jnp.sum(infobuf[:, 1, :], keepdims=True)
    stats.wait(stat)
    m4 = jnp.max(statbuf[:, 0, :], axis=0, keepdims=True)
    s4 = jnp.sum(statbuf[:, 1, :] * jnp.exp(statbuf[:, 0, :] - m4), axis=0, keepdims=True)
    lse = m4 + jnp.log(s4)
    lsend[0:1, :] = lse
    lsend[1:2, :] = jnp.sum(statbuf[:, 2, :], axis=0, keepdims=True)
    lses = Exchange('dp', 8, lsebuf, lse_s, lse_r)
    lses.start(lsend)
    lsebuf[me] = lsend[...]
    top[...] = jnp.broadcast_to(lse, (8, SEQ))
    total[...] = jnp.broadcast_to(info_ref[1:2, :] / token_count, (8, SEQ))
    across(1, plane.y, 0).start()
    gather.forward_diag(0)
    across(2, plane.diag, 0).start()

    dz_ref[...] = jnp.zeros((SEQ, WIDTH), F32)

    def backward_block(at, slot, n):
        e = eslot[slot, pl.ds(0, n), :]
        for t in range(4):
            cols = pl.ds(t * CHUNK, CHUNK)
            l = logits[pl.ds(at, n), cols].reshape(n // 8, 8, CHUNK)
            p = jnp.exp(l - top[:, cols][None])
            hit = offsets(n // 8, CHUNK) == (rows8[0, :, cols] - at)[None]
            g = (jnp.where(hit, p - 1.0, p) * total[:, cols][None]).reshape(n, CHUNK).astype(BF16)
            dz_ref[cols, :] += lax.dot_general(g, e, (((0,), (0,)), ((), ())), preferred_element_type=F32)

    blocks(backward_block, ((8, lambda: gather.forward(1)), (18, lambda: gather.forward(2))))

    for i, (lane, owner) in enumerate(((3, plane.x), (4, plane.y), (5, plane.diag))):
        across(i, owner, 3).wait_recv()
        gather.pass_on(lane, 3, owner, plane.pair)
    lses.wait(lsend)
    info_out[...] = infobuf[...]
    lse_out[...] = lsebuf[...]
    for q in (1, 2):
        gather.forward_diag(q)
    for q in range(3):
        gather.own_sent(q)
        gather.finish(q)
    gather.sent(0, 3, me)
    for lane, owner in ((0, plane.pair), (3, plane.pair_x), (4, plane.pair_y), (5, plane.pair_diag)):
        gather.arrived(lane, 3, owner)
    for i, (lane, owner) in enumerate(((3, plane.x), (4, plane.y), (5, plane.diag))):
        gather.sent(lane, 3, owner)
        across(i, owner, 0).wait_send()


def own_tokens(z, zf, embed, info):
    return pl.pallas_call(
        own_tokens_kernel,
        name='own_tokens',
        out_shape=(
            jax.ShapeDtypeStruct((8, SEQ, WIDTH), F32),
            jax.ShapeDtypeStruct((SEQ, WIDTH), F32),
            jax.ShapeDtypeStruct((8, 8, SEQ), F32),
            jax.ShapeDtypeStruct((8, 8, SEQ), F32),
        ),
        in_specs=[
            pl.BlockSpec(memory_space=pltpu.VMEM),
            pl.BlockSpec(memory_space=pl.ANY),
            pl.BlockSpec(memory_space=pl.ANY),
            pl.BlockSpec(memory_space=pltpu.VMEM),
        ],
        out_specs=(
            pl.BlockSpec(memory_space=pl.ANY),
            pl.BlockSpec(memory_space=pltpu.VMEM),
            pl.BlockSpec(memory_space=pltpu.VMEM),
            pl.BlockSpec(memory_space=pltpu.VMEM),
        ),
        scratch_shapes=[
            pltpu.VMEM((FULL * BLOCK + RESTPAD, SEQ), F32),
            pltpu.VMEM((2, BLOCK, WIDTH), BF16),
            pltpu.VMEM((8, SEQ), F32),
            pltpu.VMEM((8, SEQ), F32),
            pltpu.VMEM((8, SEQ), F32),
            pltpu.VMEM((1, 8, SEQ), jnp.int32),
            pltpu.VMEM((8, 8, SEQ), F32),
            pltpu.VMEM((8, SEQ), F32),
            pltpu.VMEM((4, 8, SEQ), F32),
            pltpu.VMEM((8, SEQ), F32),
            pltpu.VMEM((8, 8, SEQ), F32),
            pltpu.SemaphoreType.DMA((2,)),
            pltpu.SemaphoreType.DMA((3,)),
            pltpu.SemaphoreType.DMA((3,)),
            pltpu.SemaphoreType.DMA((7, 4)),
            pltpu.SemaphoreType.DMA((7, 4)),
            pltpu.SemaphoreType.DMA((8,)),
            pltpu.SemaphoreType.DMA((8,)),
            pltpu.SemaphoreType.DMA((4,)),
            pltpu.SemaphoreType.DMA((4,)),
            pltpu.SemaphoreType.DMA((8,)),
            pltpu.SemaphoreType.DMA((8,)),
        ],
        compiler_params=pltpu.CompilerParams(collective_id=1, has_side_effects=True, vmem_limit_bytes=VMEM_LIMIT),
        cost_estimate=pl.CostEstimate(flops=4 * SEQ * ROWS * WIDTH, bytes_accessed=4 * ROWS * WIDTH, transcendentals=2 * SEQ * ROWS),
    )(z, zf, embed, info)


def all_tokens_kernel(z_ref, zall_ref, e_ref, info_ref, lse_ref, dzp_ref, xhat_ref, inv_ref, gamma_ref, de_ref, dh_ref, sums_out,
                      half_in, dzh, far_in, dhh, zb, zslot, eslot, lbuf, stage_a, stage_b, lse8, scale8, rows8, sums, sum4, sumbuf4, sumbuf8,
                      half_s, half_r, far_s, far_r, dh_sem, dh_s, dh_r, z_sem, e_sem, t_sem, l_sem, gs, gr, b_s, b_r, s4_s, s4_r, s8_s, s8_r):
    plane = Plane()
    me, tp = plane.me, lax.axis_index('tp')
    enter(me, tp)

    def fetch(at, n, slot):
        return pltpu.make_async_copy(e_ref.at[pl.ds(at, n), :], eslot.at[slot, pl.ds(0, n), :], e_sem.at[slot])

    def a_at(owner, q):
        return pl.multiple_of((owner * A_STEPS + q) * A_ROWS, 16)

    def b_at(core, b):
        return pl.multiple_of(A_TOTAL + (core * B_STEPS + b) * B_ROWS, 16)

    fetch(a_at(me, 0), A_ROWS, 0).start()
    tail = pltpu.make_async_copy(e_ref.at[pl.ds(TAIL_AT, TAIL), :], eslot.at[2, pl.ds(B_ROWS, TAIL), :], t_sem)
    tail.start()

    quarters = Quarters(tp)

    def swap_with(k, partner, src, dst, send_sem, recv_sem):
        return pltpu.make_async_remote_copy(
            src_ref=src, dst_ref=dst.at[k], send_sem=send_sem.at[k], recv_sem=recv_sem.at[k],
            device_id={'tp': partner}, device_id_type=MESH)

    nears = [swap_with(k, quarters.partner[k], dzp_ref.at[pl.ds(quarters.theirs[k], CHUNK), :], half_in, half_s, half_r) for k in range(2)]
    fars = [swap_with(k, quarters.partner[1 - k], dzh.at[k], far_in, far_s, far_r) for k in range(2)]
    for near in nears:
        near.start()

    def fetch_z(n):
        owner = lax.rem(me + 1 + lax.div(n, 4), 8)
        q = pl.multiple_of(lax.rem(n, 4) * CHUNK, CHUNK)
        slot = lax.rem(n, Z_SLOTS)
        return owner, q, slot, pltpu.make_async_copy(zall_ref.at[owner, pl.ds(q, CHUNK), :], zslot.at[slot], z_sem.at[slot])

    for n in range(Z_SLOTS - 1):
        fetch_z(n)[3].start()
    zb[me] = z_ref[...]
    token_count = jnp.sum(info_ref[:, 1, :], keepdims=True)
    sub = lax.broadcasted_iota(jnp.int32, (8, SEQ), 0) + tp * ROWS
    for s in range(8):
        lse8[s] = jnp.broadcast_to(lse_ref[s, 0:1, :], (8, SEQ))
        scale8[s] = jnp.broadcast_to(info_ref[s, 1:2, :] / token_count, (8, SEQ))
        rows8[s] = jnp.broadcast_to(info_ref[s, 0:1, :].astype(jnp.int32), (8, SEQ)) - sub

    def convert(n, _):
        owner, q, slot, copy = fetch_z(n)
        copy.wait()

        @pl.when(n < 29 - Z_SLOTS)
        def _():
            fetch_z(n + Z_SLOTS - 1)[3].start()

        zb[owner, pl.ds(q, CHUNK), :] = zslot[slot].astype(BF16)
        return 0

    def logits_of(slot, n, s):
        return lax.dot_general(eslot[slot, pl.ds(0, n), :], zb[s], (((1,), (1,)), ((), ())), preferred_element_type=F32)

    def grad_of(l, n, s, at, tail_at):
        l = l.reshape(n // 8, 8, SEQ)
        p = jnp.exp(l - lse8[s][None])
        row = offsets(n // 8, SEQ) + at
        if tail_at is not None:
            row = jnp.where(offsets(n // 8, SEQ) < B_ROWS, row, row + (tail_at - B_ROWS - at))
        g = jnp.where(row == rows8[s][None], p - 1.0, p) * scale8[s][None]
        return g.reshape(n, SEQ).astype(BF16)

    def compute(slot, out, n, at, tail_at=None, arriving=False):
        lbuf[0, pl.ds(0, n), :] = logits_of(slot, n, me)
        out[...] = jnp.zeros((n, WIDTH), F32)

        def one(i, k, last):
            s = lax.rem(me + i, 8)
            if not last:
                if arriving:
                    lax.fori_loop(4 * i, 4 * i + 4, convert, 0)
                lbuf[1 - k, pl.ds(0, n), :] = logits_of(slot, n, lax.rem(me + i + 1, 8))
            g = grad_of(lbuf[k, pl.ds(0, n), :], n, s, at, tail_at)
            out[...] += jnp.dot(g, zb[s], preferred_element_type=F32)

        def pairs(i, _):
            one(2 * i, 0, False)
            one(2 * i + 1, 1, False)
            return 0

        lax.fori_loop(0, 3, pairs, 0)
        one(6, 0, False)
        one(7, 1, True)

    def region(owner, q):
        return de_ref.at[pl.ds(a_at(owner, q), A_ROWS), :]

    gather = Gather(plane, region, gs, gr)

    def keep(k, n, at):
        out = stage_a.at[k] if n == A_ROWS else stage_b.at[k - A_STEPS, pl.ds(0, n), :]
        return pltpu.make_async_copy(out, de_ref.at[pl.ds(at, n), :], l_sem.at[k])

    over_tp = Exchange('tp', 4, sumbuf4, s4_s, s4_r)

    def near_sums():
        dgamma = dbeta = jnp.zeros((8, WIDTH), F32)
        for k in range(2):
            nears[k].wait()

            def part(i, carry):
                at = pl.multiple_of(i * 64, 64)
                rows = pl.ds(pl.multiple_of(quarters.mine[k] + at, 64), 64)
                dz = dzp_ref[rows, :] + half_in[k, pl.ds(at, 64), :]
                dzh[k, pl.ds(at, 64), :] = dz
                dzx = dz * xhat_ref[rows, :]
                return carry[0] + jnp.sum(dzx.reshape(8, 8, WIDTH), axis=0), carry[1] + jnp.sum(dz.reshape(8, 8, WIDTH), axis=0)

            dgamma, dbeta = lax.fori_loop(0, CHUNK // 64, part, (dgamma, dbeta))
        sums[0:8, :] = dgamma
        sums[8:16, :] = dbeta
        over_tp.start(sums)
        for far in fars:
            far.start()
        sumbuf4[tp] = sums[...]

    def home(k):
        return pltpu.make_async_copy(dhh.at[k], dh_ref.at[pl.ds(quarters.mine[k], CHUNK), :], dh_sem.at[k])

    def swap_rows(k, rows):
        return pltpu.make_async_remote_copy(
            src_ref=dhh.at[k], dst_ref=dh_ref.at[pl.ds(rows, CHUNK), :], send_sem=dh_s.at[k], recv_sem=dh_r.at[k],
            device_id={'tp': quarters.partner[k]}, device_id_type=MESH)

    over_dp = Exchange('dp', 8, sumbuf8, s8_s, s8_r)

    def far_grads():
        over_tp.wait(sums)
        sum4[...] = sumbuf4[0] + sumbuf4[1] + sumbuf4[2] + sumbuf4[3]
        over_dp.start(sum4)
        sumbuf8[me] = sum4[...]
        for k in range(2):
            fars[k].wait()

            def part(i, _):
                at = pl.multiple_of(i * 64, 64)
                rows = pl.ds(pl.multiple_of(quarters.mine[k] + at, 64), 64)
                xh = xhat_ref[rows, :]
                g = (dzh[k, pl.ds(at, 64), :] + far_in[k, pl.ds(at, 64), :]) * gamma_ref[...]
                g = g - jnp.mean(g, axis=-1, keepdims=True) - xh * jnp.mean(g * xh, axis=-1, keepdims=True)
                dhh[k, pl.ds(at, 64), :] = g * inv_ref[rows, :]
                return 0

            lax.fori_loop(0, CHUNK // 64, part, 0)
            home(k).start()
            swap_rows(k, quarters.mine[k]).start()

    def a_step(q, _, first=False):
        slot = lax.rem(q, 2)
        fetch(a_at(me, q), A_ROWS, slot).wait()

        @pl.when(q < A_STEPS - 1)
        def _():
            fetch(a_at(me, q + 1), A_ROWS, 1 - slot).start()

        @pl.when(q == A_STEPS - 1)
        def _():
            fetch(b_at(plane.core, 0), B_ROWS, 1 - slot).start()

        if not first:
            pl.when(q == A_STEPS - 1)(near_sums)
        if first:
            compute(slot, stage_a.at[q], A_ROWS, a_at(me, q), arriving=True)
        else:
            compute(slot, stage_a.at[q], A_ROWS, a_at(me, q))
        keep(q, A_ROWS, a_at(me, q)).start()
        gather.send_own(q, stage_a.at[q])
        return 0

    a_step(0, 0, first=True)
    lax.fori_loop(1, A_STEPS, a_step, 0)

    def b_copy(b, out, core):
        at = b_at(core, b)
        return pltpu.make_async_remote_copy(
            src_ref=stage_b.at[out - A_STEPS, pl.ds(0, B_ROWS), :], dst_ref=de_ref.at[pl.ds(at, B_ROWS), :],
            send_sem=b_s.at[b], recv_sem=b_r.at[b], device_id={'dp': plane.pair}, device_id_type=MESH)

    def b_step(b, _):
        slot = lax.rem(b, 2)
        at = b_at(plane.core, b)
        fetch(at, B_ROWS, slot).wait()

        @pl.when(b < B_STEPS - 2)
        def _():
            fetch(b_at(plane.core, b + 1), B_ROWS, 1 - slot).start()

        @pl.when(b == B_STEPS - 2)
        def _():
            fetch(b_at(plane.core, B_STEPS - 1), B_ROWS, 2).start()

        gather.forward(b)
        pl.when(b == B_STEPS - 2)(lambda: gather.forward(b + 1))

        pl.when(b == B_STEPS // 2)(far_grads)
        compute(slot, stage_b.at[b, pl.ds(0, B_ROWS), :], B_ROWS, at)
        keep(A_STEPS + b, B_ROWS, at).start()
        b_copy(b, A_STEPS + b, plane.core).start()
        return 0

    lax.fori_loop(0, B_STEPS - 1, b_step, 0)

    b, slot = B_STEPS - 1, A_STEPS + B_STEPS - 1
    at = b_at(plane.core, b)
    fetch(at, B_ROWS, 2).wait()
    tail.wait()
    gather.forward_diag(0)
    gather.forward_diag(1)
    compute(2, stage_b.at[b], R_MAX, at, TAIL_AT)
    keep(slot, B_ROWS, at).start()
    b_copy(b, slot, plane.core).start()
    keep_tail = pltpu.make_async_copy(stage_b.at[b, pl.ds(B_ROWS, TAIL), :], de_ref.at[pl.ds(TAIL_AT, TAIL), :], t_sem)
    keep_tail.start()

    over_dp.wait(sum4)
    sums_out[...] = jnp.sum(sumbuf8[...], axis=0)
    for q in range(2, A_STEPS):
        gather.forward_diag(q)
    keep_tail.wait()
    for k in range(B_STEPS):
        keep(A_STEPS + k, B_ROWS, b_at(plane.core, k)).wait()
        b_copy(k, A_STEPS + k, plane.core).wait_send()
        b_copy(k, A_STEPS + k, 1 - plane.core).wait_recv()
    for k in range(2):
        home(k).wait()
        swap_rows(k, quarters.mine[k]).wait_send()
        swap_rows(k, quarters.theirs[k]).wait_recv()
    for q in range(A_STEPS):
        keep(q, A_ROWS, a_at(me, q)).wait()
        gather.own_sent(q)
        gather.finish(q)


def all_tokens(z, zall, embed, info, lse, dz, xhat, inv_std, gamma):
    return pl.pallas_call(
        all_tokens_kernel,
        name='all_tokens',
        out_shape=(
            jax.ShapeDtypeStruct((ROWS, WIDTH), F32),
            jax.ShapeDtypeStruct((SEQ, WIDTH), F32),
            jax.ShapeDtypeStruct((16, WIDTH), F32),
        ),
        in_specs=[
            pl.BlockSpec(memory_space=pltpu.VMEM),
            pl.BlockSpec(memory_space=pl.ANY),
            pl.BlockSpec(memory_space=pl.ANY),
            pl.BlockSpec(memory_space=pltpu.VMEM),
            pl.BlockSpec(memory_space=pltpu.VMEM),
            pl.BlockSpec(memory_space=pltpu.VMEM),
            pl.BlockSpec(memory_space=pltpu.VMEM),
            pl.BlockSpec(memory_space=pltpu.VMEM),
            pl.BlockSpec(memory_space=pltpu.VMEM),
        ],
        out_specs=(
            pl.BlockSpec(memory_space=pl.ANY),
            pl.BlockSpec(memory_space=pl.ANY),
            pl.BlockSpec(memory_space=pltpu.VMEM),
        ),
        scratch_shapes=[
            pltpu.VMEM((2, CHUNK, WIDTH), F32),
            pltpu.VMEM((2, CHUNK, WIDTH), F32),
            pltpu.VMEM((2, CHUNK, WIDTH), F32),
            pltpu.VMEM((2, CHUNK, WIDTH), F32),
            pltpu.VMEM((8, SEQ, WIDTH), BF16),
            pltpu.VMEM((Z_SLOTS, CHUNK, WIDTH), F32),
            pltpu.VMEM((3, R_MAX + 8, WIDTH), BF16),
            pltpu.VMEM((2, R_MAX, SEQ), F32),
            pltpu.VMEM((A_STEPS, A_ROWS, WIDTH), F32),
            pltpu.VMEM((B_STEPS, R_MAX, WIDTH), F32),
            pltpu.VMEM((8, 8, SEQ), F32),
            pltpu.VMEM((8, 8, SEQ), F32),
            pltpu.VMEM((8, 8, SEQ), jnp.int32),
            pltpu.VMEM((16, WIDTH), F32),
            pltpu.VMEM((16, WIDTH), F32),
            pltpu.VMEM((4, 16, WIDTH), F32),
            pltpu.VMEM((8, 16, WIDTH), F32),
            pltpu.SemaphoreType.DMA((2,)),
            pltpu.SemaphoreType.DMA((2,)),
            pltpu.SemaphoreType.DMA((2,)),
            pltpu.SemaphoreType.DMA((2,)),
            pltpu.SemaphoreType.DMA((2,)),
            pltpu.SemaphoreType.DMA((2,)),
            pltpu.SemaphoreType.DMA((2,)),
            pltpu.SemaphoreType.DMA((Z_SLOTS,)),
            pltpu.SemaphoreType.DMA((3,)),
            pltpu.SemaphoreType.DMA,
            pltpu.SemaphoreType.DMA((A_STEPS + B_STEPS,)),
            pltpu.SemaphoreType.DMA((7, A_STEPS)),
            pltpu.SemaphoreType.DMA((7, A_STEPS)),
            pltpu.SemaphoreType.DMA((B_STEPS,)),
            pltpu.SemaphoreType.DMA((B_STEPS,)),
            pltpu.SemaphoreType.DMA((4,)),
            pltpu.SemaphoreType.DMA((4,)),
            pltpu.SemaphoreType.DMA((8,)),
            pltpu.SemaphoreType.DMA((8,)),
        ],
        compiler_params=pltpu.CompilerParams(collective_id=2, has_side_effects=True, vmem_limit_bytes=VMEM_LIMIT),
        cost_estimate=pl.CostEstimate(flops=32 * SEQ * 3200 * WIDTH, bytes_accessed=8 * ROWS * WIDTH, transcendentals=8 * SEQ * 3200),
    )(z, zall, embed, info, lse, dz, xhat, inv_std, gamma)


def solution(mesh):
    def local_step(hidden, ln_gamma, ln_beta, embed_shard, labels, loss_mask):
        shard_start = lax.axis_index('tp') * ROWS
        x_hat, inv_std, normed = layer_norm_fwd(hidden[0], ln_gamma, ln_beta)
        z = normed.astype(BF16)
        here = labels - shard_start
        here = jnp.where((here >= 0) & (here < ROWS), here, -1)
        info = jnp.concatenate([labels.astype(F32), loss_mask.astype(F32), here.astype(F32), jnp.zeros((5, SEQ), F32)], axis=0)
        zall, dz_part, info_all, lse_all = own_tokens(z, z.astype(F32), embed_shard, info)
        d_embed, d_rows, sums = all_tokens(z, zall, embed_shard, info_all, lse_all, dz_part, x_hat, inv_std, ln_gamma[None])
        mask = info_all[:, 1, :]
        mean_loss = jnp.sum(mask * (lse_all[:, 0, :] - lse_all[:, 1, :])) / jnp.sum(mask)
        d_gamma = jnp.sum(sums[:8], axis=0)
        d_beta = jnp.sum(sums[8:], axis=0)
        d_hidden = d_rows.astype(BF16)[None]
        return mean_loss, d_hidden, d_embed, d_gamma, d_beta

    return jax.shard_map(local_step, mesh=mesh, in_specs=(P('dp', None, None), P(None), P(None), P('tp', None), P('dp', None), P('dp', None)), out_specs=(P(), P('dp', None, None), P('tp', None), P(None), P(None)), check_vma=False)
```
